512 devices in a mesh: dp: 16 (over z_lo, y), expert: 32 (over x, z_hi, core).
Axes of the slice: x: 4, y: 8, z: 8 (z_hi: 4, z_lo: 2; z = z_hi * 2 + z_lo), core: 2. Of those that a mesh axis runs over, the one named last changes fastest.
Arguments:
- tokens: bfloat16 [32768, 2560], P(('dp', 'expert')), may hold values from -6 to 6
- expert_ids: int32 [32768, 6], P(('dp', 'expert')), may hold values from 0 to 31, all different within a row; in each aligned block of 64 rows (0 to 63, 64 to 127, ...) at most 16 rows name the same one
- gate_scores: float32 [32768, 6], P(('dp', 'expert')), may hold values from 0.02 to 0.4
- w_gate: bfloat16 [32, 2560, 768], P('expert', 'dp'), may hold values from -0.125 to 0.125
- w_up: bfloat16 [32, 2560, 768], P('expert', 'dp'), may hold values from -0.125 to 0.125
- w_down: bfloat16 [32, 768, 2560], P('expert', None, 'dp'), may hold values from -0.21875 to 0.21875
Outputs:
- mixed: bfloat16 [32768, 2560], P(('dp', 'expert'))
- expert_load: int32 [32], P('expert')
- balance_loss: float32 [], replicated
The draws below stay inside these ranges and needn't reach their ends.
Inputs may be any that keep to these rules, and one draw needn't show every extreme that they name: `expert_ids`: each row names 6 different experts. The rows of one device name any one expert at most 16 times, and in every draw some device names some expert exactly 16 times.
All inputs are finite; a program needn't handle non-finite values.
Results may differ from the reference program's by a relative error of at most 0.0085.
Values may be sent and summed in bfloat16 or wider, within the bound.
A program may use at most 64 MiB of HBM per device.

```python
import math
import jax
import jax.numpy as jnp
import numpy as np
from jax import lax

D = 2560
HID = 768
TOPK = 6
TOK_DEV = 64
EXPERTS = 32
CAP = 16
TOKENS = 32768


def block_levels(stream_key, shape, pieces, smallest, largest):
    gain, own = 1.0, jax.random.fold_in(stream_key, 6)
    for dim, blocks in pieces:
        draws = jnp.exp(jax.random.uniform(jax.random.fold_in(own, dim), (blocks,), jnp.float32, smallest / len(pieces), largest / len(pieces)))
        gain = gain * jnp.repeat(draws, shape[dim] // blocks).reshape([-1 if axis == dim else 1 for axis in range(len(shape))])
    return gain


def routed_block(rng, own, number, rows, amount, top, reach, lean):
    sequence = jax.random.permutation(rng, amount)
    heavy_load, common = shares(amount, rows * top, reach, lean, True), shares(amount, rows * top, reach, lean, False)
    places = jnp.arange(amount)

    def named(lengths, offset_by):
        used = int((lengths > 0).sum())
        fixed = max(1, used // 4)
        passed = fixed + (places - fixed + offset_by * (used - fixed)) % max(1, amount - fixed)
        return jnp.zeros((amount,), jnp.int32).at[sequence[jnp.where(places < fixed, places, passed)]].set(jnp.asarray(lengths, jnp.int32))

    lengths = jnp.where(number % 4 == 0, named(heavy_load, number // 4), named(common, number - number // 4 - 1))
    mixed = jax.random.permutation(jax.random.fold_in(own, 3), amount)
    giver, sink = mixed[0:amount // 2 * 2:2], mixed[1:amount // 2 * 2:2]
    room = jnp.minimum(lengths[giver] - 1, reach - lengths[sink]) // 2
    room = jnp.where((giver == sequence[0]) | (sink == sequence[0]) | (lengths[sink] == 0), 0, jnp.maximum(room, 0))
    passed = jax.random.randint(jax.random.fold_in(own, 4), (amount // 2,), 0, 1 << 20) % (room + 1)
    lengths = lengths.at[giver].add(-passed).at[sink].add(passed)
    labels = jnp.searchsorted(jnp.cumsum(lengths), jnp.arange(rows * top), side="right").astype(jnp.int32)
    table = labels.reshape(top, rows).T
    table = table[jax.random.permutation(jax.random.fold_in(own, 1), rows)]
    offset_by = jax.random.randint(jax.random.fold_in(own, 2), (rows, 1), 0, top)
    return jnp.take_along_axis(table, (jnp.arange(top)[None, :] + offset_by) % top, axis=1)


def shares(number_of, total, bound, lean, full):
    portions = [(1 << 20) // math.isqrt(rank ** lean) + 1 for rank in range(1, number_of + 1)]
    largest = bound if full else min(bound, max(-(-total // number_of), total * portions[0] // sum(portions)))
    least = 1 if total - largest >= number_of - 1 else 0
    holding, spare = [largest] + [least] * (number_of - 1), total - largest - least * (number_of - 1)
    while spare > 0:
        movable = [i for i in range(1, number_of) if holding[i] < largest] or [i for i in range(1, number_of) if holding[i] < bound]
        pool, remaining = sum([portions[i] for i in movable]), spare
        for i in movable:
            addition = min(bound - holding[i], max(1, remaining * portions[i] // pool), spare)
            holding[i] = holding[i] + addition
            spare = spare - addition
    return np.array(holding)


def bell_draw(rng, dims, scale, bound, shards=(), kind=jnp.bfloat16):
    entries = scale * jax.random.normal(rng, dims, jnp.float32)
    if shards:
        entries = entries * block_levels(rng, dims, shards, -0.22, 0.18)
    return jnp.clip(entries, -bound, bound).astype(kind)


def setup_inputs(seed: int = 0) -> dict:
    key_list = jax.random.split(jax.random.key(seed), 7)
    tokens = bell_draw(key_list[0], (TOKENS, D), 1.0, 6.0, ((0, 512),))
    expert_ids_keys = jax.random.split(jax.random.fold_in(key_list[1], 1), TOKENS // TOK_DEV)
    expert_ids_turns = jax.random.permutation(jax.random.fold_in(key_list[1], 3), TOKENS // TOK_DEV)
    expert_ids = jax.vmap(lambda own, number: routed_block(jax.random.fold_in(key_list[1], 2), own, number, TOK_DEV, EXPERTS, TOPK, CAP, 2))(expert_ids_keys, expert_ids_turns).reshape((TOKENS, TOPK))
    gate_scores = jnp.clip(jnp.exp(math.log(0.4) - 2.9957323 * jax.random.uniform(key_list[2], (TOKENS, TOPK), jnp.float32) ** block_levels(key_list[2], (TOKENS, TOPK), ((0, 512),), -0.2, 0.2)), 0.02, 0.4)
    w_gate = bell_draw(key_list[3], (EXPERTS, D, HID), D ** -0.5, 0.125, ((0, 32), (1, 16)))
    w_up = bell_draw(key_list[4], (EXPERTS, D, HID), D ** -0.5, 0.125, ((0, 32), (1, 16)))
    w_down = bell_draw(key_list[5], (EXPERTS, HID, D), HID ** -0.5, 0.21875, ((0, 32), (2, 16)))
    return {"tokens": tokens, "expert_ids": expert_ids, "gate_scores": gate_scores, "w_gate": w_gate, "w_up": w_up, "w_down": w_down}


def reference(tokens, expert_ids, gate_scores, w_gate, w_up, w_down):
    total, width = tokens.shape
    experts = w_gate.shape[0]
    blocks = total // TOK_DEV
    pairs = TOK_DEV * TOPK
    block_ids = expert_ids.reshape(blocks, pairs)
    onehot = (block_ids[:, :, None] == jnp.arange(experts, dtype=jnp.int32)[None, None, :]).astype(jnp.int32)
    ranks = jnp.cumsum(onehot, axis=1) - onehot
    slot_of = jnp.sum(ranks * onehot, axis=2).astype(jnp.int32)
    block_of = jnp.broadcast_to(jnp.arange(blocks, dtype=jnp.int32)[:, None], (blocks, pairs))
    token_of = block_of * TOK_DEV + (jnp.arange(pairs, dtype=jnp.int32) // TOPK)[None, :]
    table = jnp.full((experts, blocks, CAP), -1, jnp.int32)
    table = table.at[block_ids, block_of, slot_of].set(token_of)
    slot_tok = slot_of.reshape(total, TOPK)
    row_base = (jnp.arange(total, dtype=jnp.int32) // TOK_DEV) * CAP

    def per_expert(carry, inputs):
        index, gate_w, up_w, down_w, sources = inputs
        live = sources >= 0
        rows = jnp.where(live[:, None], tokens[jnp.maximum(sources, 0)], jnp.zeros((), tokens.dtype))
        gate = jnp.dot(rows, gate_w, preferred_element_type=jnp.float32)
        up = jnp.dot(rows, up_w, preferred_element_type=jnp.float32)
        hidden = (jax.nn.silu(gate) * up).astype(jnp.bfloat16)
        produced = jnp.dot(hidden, down_w, preferred_element_type=jnp.float32).astype(jnp.bfloat16)
        match = expert_ids == index
        weight = jnp.sum(jnp.where(match, gate_scores, jnp.zeros((), gate_scores.dtype)), axis=1)
        slot = jnp.sum(jnp.where(match, slot_tok, 0), axis=1).astype(jnp.int32)
        picked = produced[row_base + slot].astype(jnp.float32)
        return carry + weight[:, None] * picked, None

    mixed, _ = lax.scan(per_expert, jnp.zeros((total, width), jnp.float32),
                        (jnp.arange(experts, dtype=jnp.int32), w_gate, w_up, w_down,
                         table.reshape(experts, blocks * CAP)))
    load = jnp.sum(onehot, axis=(0, 1)).astype(jnp.int32)
    mass = jnp.sum(onehot.astype(jnp.float32) * gate_scores.reshape(blocks, pairs)[:, :, None], axis=(0, 1))
    load_f = load.astype(jnp.float32)
    balance_loss = jnp.sum((experts * load_f / (TOPK * total)) * (mass / total))
    return mixed.astype(jnp.bfloat16), load, balance_loss
```

```python
import functools

import jax
import jax.numpy as jnp
from jax import lax
from jax.experimental import pallas as pl
from jax.experimental.pallas import tpu as pltpu
from jax.sharding import PartitionSpec as P

F32, BF16, I32 = jnp.float32, jnp.bfloat16, jnp.int32
X, ZH, C, ZL, Y = 4, 4, 2, 2, 8
CAP = 16
XC = X * C
EXPERTS = X * ZH * C
GROUPS = ZL * Y
CHUNKS = 4
RIGHT, LEFT = 1, -1


def iota(shape, dim):
    return lax.broadcasted_iota(I32, shape, dim)


def dot(a, b):
    return jnp.dot(a, b, preferred_element_type=F32)


def remote(src, dst, send, recv, dp, ex):
    return pltpu.make_async_remote_copy(
        src_ref=src,
        dst_ref=dst,
        send_sem=send,
        recv_sem=recv,
        device_id=(dp, ex),
        device_id_type=pl.DeviceIdType.MESH,
    )


def expert_of(xc, zh):
    return ((xc >> 1) * ZH + zh) * C + (xc & 1)


def expert_index(x, zh, core):
    return (x * ZH + zh) * C + core


def ring_messages(direction):
    far = "g" if direction == RIGHT else "u"
    half = 0 if direction == RIGHT else 1
    out = []
    for z in (0, 1):
        for hops in range(3):
            out += [("g", z, hops, 0, 2), ("u", z, hops, 0, 2)]
        out.append((far, z, 3, 0, 2))
    for z in (0, 1):
        out += [("d", z, 0, 0, 1), ("d", z, 0, 1, 1)]
    for z in (0, 1):
        for hops in (1, 2):
            out += [("d", z, hops, 0, 1), ("d", z, hops, 1, 1)]
        out.append(("d", z, 3, half, 1))
    return out


MESSAGES = len(ring_messages(RIGHT))
GATE_UP = 14


def kernel(
    tokens,
    ids,
    scores,
    wg,
    wu,
    wd,
    out,
    stat_out,
    gate_w,
    up_w,
    down_w,
    outgoing,
    rows,
    hidden,
    produced,
    x_in,
    partial,
    z_in,
    w_send,
    w_recv,
    w_wide,
    stat_a,
    stat_b,
    stat_mine,
    ring_send,
    ring_recv,
    zx_send,
    zx_recv,
    row_send,
    row_recv,
    w_ssem,
    w_rsem,
    sa_send,
    sa_recv,
    sb_send,
    sb_recv,
    xp_send,
    xp_recv,
    zp_send,
    zp_recv,
):
    toks, width = tokens.shape
    piece, hid = wg.shape
    half = piece // 2
    slots = EXPERTS * CAP
    span = width // CHUNKS

    dp = lax.axis_index("dp")
    me = lax.axis_index("expert")
    zl, y = dp // Y, dp % Y
    core, zh, x = me % C, (me // C) % ZH, me // (C * ZH)
    xc = x * C + core
    pos = xc * ZH + zh
    partner = (1 - zl) * Y + y

    barrier = pltpu.get_barrier_semaphore()

    def greet_expert(k, carry):
        pl.semaphore_signal(
            barrier, inc=1, device_id=(dp, (me + k) % EXPERTS), device_id_type=pl.DeviceIdType.MESH
        )
        return carry

    def greet_group(k, carry):
        pl.semaphore_signal(
            barrier, inc=1, device_id=((dp + k) % GROUPS, me), device_id_type=pl.DeviceIdType.MESH
        )
        return carry

    lax.fori_loop(1, GROUPS, greet_group, 0)
    lax.fori_loop(1, EXPERTS, greet_expert, 0)

    lanes = 128
    expert_lane = iota((toks, lanes), 1)
    named = jnp.zeros((toks, lanes), F32)
    score = jnp.zeros((toks, lanes), F32)
    for k in range(ids.shape[1]):
        hit = ids[:, k : k + 1] == expert_lane
        named = named + jnp.where(hit, 1.0, 0.0)
        score = score + jnp.where(hit, scores[:, k : k + 1], 0.0)
    earlier = (iota((toks, toks), 0) > iota((toks, toks), 1)).astype(F32).astype(BF16)
    named16 = named.astype(BF16)
    rank = dot(earlier, named16)
    rank16 = rank.astype(BF16)
    score_high = score.astype(BF16)
    score_low = (score - score_high.astype(F32)).astype(BF16)

    slot_expert = iota((lanes, slots), 1) >> 4
    spread = (iota((lanes, slots), 0) == slot_expert).astype(F32).astype(BF16)
    place = jnp.where(
        dot(rank16, spread) == (iota((toks, slots), 1) & 15).astype(F32), dot(named16, spread), 0.0
    ).astype(BF16)

    load = jnp.sum(named, axis=0, keepdims=True)
    mass = jnp.sum(score, axis=0, keepdims=True)
    row8 = iota((8, lanes), 0)
    stat_mine[0] = jnp.where(row8 == 0, load, jnp.where(row8 == 1, mass, 0.0))

    wide = 128
    slot_wide = (iota((toks, wide), 1) & 15).astype(F32)
    for z in range(ZH):
        pick = (iota((lanes, wide), 0) == expert_of(iota((lanes, wide), 1) >> 4, z)).astype(F32).astype(BF16)
        there = dot(rank16, pick) == slot_wide
        w_send[z, 0] = jnp.where(there, dot(score_high, pick), 0.0).astype(BF16)
        w_send[z, 1] = jnp.where(there, dot(score_low, pick), 0.0).astype(BF16)

    pl.semaphore_wait(barrier, EXPERTS - 1 + GROUPS - 1)

    full = {"g": gate_w, "u": up_w, "d": down_w}
    own = {"g": wg, "u": wu, "d": wd}

    def region(array, z, at, first, count):
        group = (zl if z == 0 else 1 - zl) * Y + at
        return full[array].at[pl.ds(pl.multiple_of(group * piece + first * half, 16), count * half), :]

    order = {RIGHT: ring_messages(RIGHT), LEFT: ring_messages(LEFT)}
    index = {s: {m[:4]: n for n, m in enumerate(order[s])} for s in order}
    side = {RIGHT: 0, LEFT: 1}
    arrived, started, zx_done = set(), [], set()
    zx = {}

    def start_zx(array):
        n = "gud".index(array)
        c = remote(
            own[array], region(array, 0, y, 0, 2), zx_send.at[n], zx_recv.at[n], partner, me
        )
        c.start()
        zx[array] = c

    def wait_zx(array):
        if array not in zx_done:
            zx_done.add(array)
            n = "gud".index(array)
            there = region(array, 1, y, 0, 2)
            remote(there, there, zx_send.at[n], zx_recv.at[n], partner, me).wait_recv()

    def wait_ring(s, n):
        if (s, n) in arrived:
            return
        arrived.add((s, n))
        array, z, hops, first, count = order[s][n]
        there = region(array, z, (y - s * (hops + 1) + 2 * Y) % Y, first, count)
        remote(
            there, there, ring_send.at[side[s], n], ring_recv.at[side[s], n], dp, me
        ).wait_recv()

    def forward(s, n):
        array, z, hops, first, count = order[s][n]
        at = (y - s * hops + 2 * Y) % Y
        if hops:
            if (array, z, hops - 1, first) in index[s]:
                wait_ring(s, index[s][(array, z, hops - 1, first)])
        elif z:
            wait_zx(array)
        if hops == 0 and z == 0:
            src = own[array].at[pl.ds(first * half, count * half), :]
        else:
            src = region(array, z, at, first, count)
        c = remote(
            src,
            region(array, z, at, first, count),
            ring_send.at[side[s], n],
            ring_recv.at[side[s], n],
            zl * Y + (y + s + Y) % Y,
            me,
        )
        c.start()
        started.append(c)

    def ring_step(n):
        forward(RIGHT, n)
        forward(LEFT, n)

    start_zx("g")
    start_zx("u")
    ring_step(0)
    ring_step(1)

    def send_part(k, carry):
        at = pl.ds(pl.multiple_of(k * 512, 512), 512)
        outgoing[:, at] = lax.dot_general(
            place, tokens[:, at], (((0,), (0,)), ((), ())), preferred_element_type=F32
        ).astype(BF16)
        return carry

    lax.fori_loop(0, width // 512, send_part, 0)

    def row_block(ref, n):
        return ref.at[pl.ds(pl.multiple_of(n * CAP, CAP), CAP), :]

    def row_copy(k):
        to = (me + k) % EXPERTS
        return remote(row_block(outgoing, to), row_block(rows, pos), row_send.at[k], row_recv.at[k], dp, to)

    def row_start(k, carry):
        row_copy(k).start()
        return carry

    def row_wait(k, carry):
        source = (me - k + EXPERTS) % EXPERTS
        place_of = ((source // (C * ZH)) * C + source % C) * ZH + (source // C) % ZH
        there = row_block(rows, place_of)
        remote(there, there, row_send.at[k], row_recv.at[k], dp, me).wait_recv()
        return carry

    def row_sent(k, carry):
        row_copy(k).wait_send()
        return carry

    def w_copy(k):
        to = (zh + k) % ZH
        return remote(w_send.at[to], w_recv.at[zh], w_ssem.at[k], w_rsem.at[k], dp, expert_index(x, to, core))

    def stat_a_copy(k):
        to = (dp + k) % GROUPS
        return remote(stat_mine.at[0], stat_a.at[dp], sa_send.at[k], sa_recv.at[k], to, me)

    def stat_b_copy(k):
        to = (me + k) % EXPERTS
        return remote(stat_mine.at[1], stat_b.at[me], sb_send.at[k], sb_recv.at[k], dp, to)

    def starts(copy, count):
        def one(k, carry):
            copy(k).start()
            return carry

        lax.fori_loop(1, count, one, 0)

    def sent(copy, count):
        def one(k, carry):
            copy(k).wait_send()
            return carry

        lax.fori_loop(1, count, one, 0)

    starts(stat_a_copy, GROUPS)
    for k in range(1, ZH):
        w_copy(k).start()
    lax.fori_loop(1, EXPERTS, row_start, 0)
    start_zx("d")
    stat_a[dp] = stat_mine[0]
    w_recv[zh] = w_send[zh]
    mine = pl.ds(pl.multiple_of(dp * piece, 16), piece)
    rows[pl.ds(pl.multiple_of(pos * CAP, CAP), CAP), :] = outgoing[
        pl.ds(pl.multiple_of(me * CAP, CAP), CAP), :
    ]
    gate_w[mine, :] = wg[...]
    up_w[mine, :] = wu[...]
    down_w[mine, :] = wd[...]

    ring_step(2)
    ring_step(3)

    def stat_a_wait(k, carry):
        there = stat_a.at[(dp - k + GROUPS) % GROUPS]
        remote(there, there, sa_send.at[k], sa_recv.at[k], dp, me).wait_recv()
        return carry

    lax.fori_loop(1, GROUPS, stat_a_wait, 0)
    stat_mine[1] = jnp.sum(stat_a[...], axis=0)
    starts(stat_b_copy, EXPERTS)
    stat_b[me] = stat_mine[1]

    for n in range(4, 10):
        ring_step(n)

    def stat_b_wait(k, carry):
        there = stat_b.at[(me - k + EXPERTS) % EXPERTS]
        remote(there, there, sb_send.at[k], sb_recv.at[k], dp, me).wait_recv()
        return carry

    lax.fori_loop(1, EXPERTS, stat_b_wait, 0)
    totals = jnp.sum(stat_b[...], axis=0)
    count, masses = totals[0:1, :], totals[1:2, :]
    total = toks * GROUPS * EXPERTS
    loss = jnp.sum(
        (EXPERTS * count / (ids.shape[1] * total)) * (masses / total), axis=1, keepdims=True
    )
    my_load = jnp.sum(jnp.where(iota((1, lanes), 1) == me, count, 0.0), axis=1, keepdims=True)
    stat_out[...] = jnp.where(row8 == 0, my_load, jnp.where(row8 == 1, loss, 0.0))

    for k in range(1, ZH):
        there = w_recv.at[(zh - k + ZH) % ZH]
        remote(there, there, w_ssem.at[k], w_rsem.at[k], dp, me).wait_recv()
    from_slot, to_slot = iota((wide, slots), 0), iota((wide, slots), 1)
    for z in range(ZH):
        widen = (
            ((to_slot >> 6) == (from_slot >> 4))
            & (((to_slot >> 4) & 3) == z)
            & ((to_slot & 15) == (from_slot & 15))
        )
        widen = widen.astype(F32).astype(BF16)
        for part in range(2):
            w_wide[pl.ds((part * ZH + z) * toks, toks), :] = dot(w_recv[z, part], widen).astype(BF16)

    for n in range(10, 18):
        ring_step(n)

    lax.fori_loop(1, EXPERTS, row_wait, 0)
    for s in (RIGHT, LEFT):
        for n in range(GATE_UP):
            wait_ring(s, n)

    part_width = 256
    block = slots // 2
    for n in range(hid // part_width):
        columns = slice(n * part_width, (n + 1) * part_width)

        def hidden_rows(m, carry, columns=columns):
            at = pl.ds(pl.multiple_of(m * block, block), block)
            gate = dot(rows[at, :], gate_w[:, columns])
            up = dot(rows[at, :], up_w[:, columns])
            hidden[at, columns] = (gate / (1.0 + jnp.exp(-gate)) * up).astype(BF16)
            return carry

        lax.fori_loop(0, slots // block, hidden_rows, 0)
        if n:
            ring_step(17 + n)

    def chunk_start(n):
        z = zl if n < 2 else 1 - zl
        return pl.multiple_of((z * 2 + n % 2) * span, span)

    def x_block(ref, n, at):
        return ref.at[n, pl.ds(pl.multiple_of(at * ZH * CAP, ZH * CAP), ZH * CAP), :]

    def x_copy(n):
        def copy(k):
            to = (xc + k) % XC
            return remote(
                x_block(produced, n, to),
                x_block(x_in, n, xc),
                xp_send.at[n, k],
                xp_recv.at[n, k],
                dp,
                expert_index(to // C, zh, to % C),
            )

        return copy

    def z_copy(n):
        def copy(k):
            to = (zh + k) % ZH
            return remote(
                partial.at[n, to],
                z_in.at[n, zh],
                zp_send.at[n, k],
                zp_recv.at[n, k],
                dp,
                expert_index(x, to, core),
            )

        return copy

    def produce(n):
        produced[n] = lax.dot_general(
            hidden[...],
            down_w[pl.ds(chunk_start(n), span), :],
            (((1,), (1,)), ((), ())),
            preferred_element_type=F32,
        ).astype(BF16)
        starts(x_copy(n), XC)
        at = pl.ds(pl.multiple_of(xc * ZH * CAP, ZH * CAP), ZH * CAP)
        x_in[n, at, :] = produced[n, at, :]

    def combine(n):
        def wait(k, carry):
            there = x_block(x_in, n, (xc - k + XC) % XC)
            remote(there, there, xp_send.at[n, k], xp_recv.at[n, k], dp, me).wait_recv()
            return carry

        lax.fori_loop(1, XC, wait, 0)
        both = dot(w_wide[...], x_in[n])
        summed = (both[: ZH * toks] + both[ZH * toks :]).astype(BF16)
        for z in range(ZH):
            partial[n, z] = summed[z * toks : (z + 1) * toks]
        starts(z_copy(n), ZH)
        z_in[n, zh] = partial[n, zh]

    def finish(n):
        def wait(k, carry):
            there = z_in.at[n, (zh - k + ZH) % ZH]
            remote(there, there, zp_send.at[n, k], zp_recv.at[n, k], dp, me).wait_recv()
            return carry

        lax.fori_loop(1, ZH, wait, 0)
        result = z_in[n, 0].astype(F32)
        for z in range(1, ZH):
            result = result + z_in[n, z].astype(F32)
        out[:, pl.ds(chunk_start(n), span)] = result.astype(BF16)

    def wait_down(z):
        for s in (RIGHT, LEFT):
            for n in range(GATE_UP, MESSAGES):
                if order[s][n][1] == z:
                    wait_ring(s, n)

    for n in range(20, 23):
        ring_step(n)
    wait_down(0)
    produce(0)
    ring_step(23)
    ring_step(24)
    produce(1)
    ring_step(25)
    ring_step(26)
    combine(0)
    ring_step(27)
    combine(1)
    wait_zx("d")
    wait_down(1)
    produce(2)
    produce(3)
    finish(0)
    finish(1)
    combine(2)
    combine(3)
    finish(2)
    finish(3)

    for c in started:
        c.wait_send()
    for array in "gud":
        zx[array].wait_send()
    for k in range(1, ZH):
        w_copy(k).wait_send()
    lax.fori_loop(1, EXPERTS, row_sent, 0)
    sent(stat_a_copy, GROUPS)
    sent(stat_b_copy, EXPERTS)
    for n in range(CHUNKS):
        sent(x_copy(n), XC)
        sent(z_copy(n), ZH)


def on_device(tokens, expert_ids, gate_scores, w_gate, w_up, w_down):
    toks, width = tokens.shape
    hid = w_gate.shape[2]
    slots = EXPERTS * CAP
    span = width // CHUNKS
    dma = pltpu.SemaphoreType.DMA
    vmem = pl.BlockSpec(memory_space=pltpu.VMEM)
    mixed, stats = pl.pallas_call(
        kernel,
        out_shape=(
            jax.ShapeDtypeStruct((toks, width), BF16),
            jax.ShapeDtypeStruct((8, 128), F32),
        ),
        in_specs=[vmem] * 6,
        out_specs=(vmem, vmem),
        scratch_shapes=[
            pltpu.VMEM((width, hid), BF16),
            pltpu.VMEM((width, hid), BF16),
            pltpu.VMEM((width, hid), BF16),
            pltpu.VMEM((slots, width), BF16),
            pltpu.VMEM((slots, width), BF16),
            pltpu.VMEM((slots, hid), BF16),
            pltpu.VMEM((CHUNKS, slots, span), BF16),
            pltpu.VMEM((CHUNKS, slots, span), BF16),
            pltpu.VMEM((CHUNKS, ZH, toks, span), BF16),
            pltpu.VMEM((CHUNKS, ZH, toks, span), BF16),
            pltpu.VMEM((ZH, 2, toks, 128), BF16),
            pltpu.VMEM((ZH, 2, toks, 128), BF16),
            pltpu.VMEM((2 * ZH * toks, slots), BF16),
            pltpu.VMEM((GROUPS, 8, 128), F32),
            pltpu.VMEM((EXPERTS, 8, 128), F32),
            pltpu.VMEM((2, 8, 128), F32),
            dma((2, MESSAGES)),
            dma((2, MESSAGES)),
            dma((3,)),
            dma((3,)),
            dma((EXPERTS,)),
            dma((EXPERTS,)),
            dma((ZH,)),
            dma((ZH,)),
            dma((GROUPS,)),
            dma((GROUPS,)),
            dma((EXPERTS,)),
            dma((EXPERTS,)),
            dma((CHUNKS, XC)),
            dma((CHUNKS, XC)),
            dma((CHUNKS, ZH)),
            dma((CHUNKS, ZH)),
        ],
        compiler_params=pltpu.CompilerParams(
            collective_id=0, has_side_effects=True, vmem_limit_bytes=60 * 1024 * 1024
        ),
        name="routed_layer",
    )(tokens, expert_ids, gate_scores, w_gate[0], w_up[0], w_down[0].T)
    return mixed, stats[0, :1].astype(I32), stats[1, 0]


def solution(mesh):
    both = ("dp", "expert")
    return jax.shard_map(
        on_device,
        mesh=mesh,
        in_specs=(
            P(both, None),
            P(both, None),
            P(both, None),
            P("expert", "dp", None),
            P("expert", "dp", None),
            P("expert", None, "dp"),
        ),
        out_specs=(P(both, None), P("expert"), P()),
        check_vma=False,
    )
```

```python
import functools

import jax
import jax.numpy as jnp
from jax import lax
from jax.experimental import pallas as pl
from jax.experimental.pallas import tpu as pltpu
from jax.sharding import PartitionSpec as P

F32, BF16, I32 = jnp.float32, jnp.bfloat16, jnp.int32
X, ZH, C, ZL, Y = 4, 4, 2, 2, 8
CAP = 16
XC = X * C
EXPERTS = X * ZH * C
GROUPS = ZL * Y
RIGHT, LEFT = 1, -1
CHUNKS = (
    (0, 0, 384),
    (1, 0, 384),
    (0, 384, 256),
    (1, 384, 256),
    (0, 1024, 256),
    (0, 640, 384),
    (1, 1024, 256),
    (1, 640, 256),
    (1, 896, 128),
)


def iota(shape, dim):
    return lax.broadcasted_iota(I32, shape, dim)


def dot(a, b):
    return jnp.dot(a, b, preferred_element_type=F32)


def dot_down(a, b):
    return lax.dot_general(a, b, (((0,), (0,)), ((), ())), preferred_element_type=F32)


def dot_across(a, b):
    return lax.dot_general(a, b, (((1,), (1,)), ((), ())), preferred_element_type=F32)


def remote(src, dst, send, recv, dp, ex):
    return pltpu.make_async_remote_copy(
        src_ref=src,
        dst_ref=dst,
        send_sem=send,
        recv_sem=recv,
        device_id=(dp, ex),
        device_id_type=pl.DeviceIdType.MESH,
    )


def expert_of(xc, zh):
    return ((xc >> 1) * ZH + zh) * C + (xc & 1)


def expert_index(x, zh, core):
    return (x * ZH + zh) * C + core


def ring_messages(direction):
    far = "g" if direction == RIGHT else "u"
    half = 0 if direction == RIGHT else 1
    out = []
    for z in (0, 1):
        for hops in range(3):
            out += [("g", z, hops, 0, 2), ("u", z, hops, 0, 2)]
        out.append((far, z, 3, 0, 2))
    for hops in (0, 1):
        for z in (0, 1):
            out += [("d", z, hops, 0, 1), ("d", z, hops, 1, 1)]
    out += [("d", 0, 2, half, 1), ("d", 0, 2, 1 - half, 1)]
    out += [("d", 1, 2, half, 1), ("d", 0, 3, half, 1)]
    out += [("d", 1, 2, 1 - half, 1), ("d", 1, 3, half, 1)]
    return out


MESSAGES = len(ring_messages(RIGHT))
GATE_UP = 14


def kernel(
    tokens,
    ids,
    scores,
    wg,
    wu,
    wd,
    out,
    stat_out,
    gate_w,
    up_w,
    down_w,
    outgoing,
    rows,
    hidden,
    relative,
    w_send,
    w_recv,
    w_wide,
    stat_a,
    stat_b,
    stat_mine,
    ring_send,
    ring_recv,
    zx_send,
    zx_recv,
    row_send,
    row_recv,
    w_ssem,
    w_rsem,
    sa_send,
    sa_recv,
    sb_send,
    sb_recv,
    xp_send,
    xp_recv,
    zp_send,
    zp_recv,
    *chunk_buffers,
):
    produced, x_in, partial, z_in = (
        chunk_buffers[n * len(CHUNKS) : (n + 1) * len(CHUNKS)] for n in range(4)
    )
    toks, width = tokens.shape
    piece, hid = wg.shape
    half = piece // 2
    slots = EXPERTS * CAP
    topk = ids.shape[0]

    dp = lax.axis_index("dp")
    me = lax.axis_index("expert")
    zl, y = dp // Y, dp % Y
    core, zh, x = me % C, (me // C) % ZH, me // (C * ZH)
    xc = x * C + core
    pos = xc * ZH + zh
    partner = (1 - zl) * Y + y

    barrier = pltpu.get_barrier_semaphore()

    def greet_expert(k, carry):
        pl.semaphore_signal(
            barrier, inc=1, device_id=(dp, (me + k) % EXPERTS), device_id_type=pl.DeviceIdType.MESH
        )
        return carry

    def greet_group(k, carry):
        pl.semaphore_signal(
            barrier, inc=1, device_id=((dp + k) % GROUPS, me), device_id_type=pl.DeviceIdType.MESH
        )
        return carry

    lax.fori_loop(1, GROUPS, greet_group, 0)
    lax.fori_loop(1, EXPERTS, greet_expert, 0)

    lanes = 128
    expert_row = iota((lanes, toks), 0)
    named = jnp.zeros((lanes, toks), F32)
    score = jnp.zeros((lanes, toks), F32)
    for k in range(topk):
        hit = ids[k : k + 1, :] == expert_row
        named = named + jnp.where(hit, 1.0, 0.0)
        score = score + jnp.where(hit, scores[k : k + 1, :], 0.0)
    earlier = (iota((toks, toks), 0) < iota((toks, toks), 1)).astype(F32).astype(BF16)
    named16 = named.astype(BF16)
    rank16 = dot(named16, earlier).astype(BF16)
    score_high = score.astype(BF16)
    rest = score - score_high.astype(F32)
    score_low = rest.astype(BF16)
    score_last = (rest - score_low.astype(F32)).astype(BF16)

    ones = jnp.ones((8, toks), BF16)
    load = dot_across(ones, named16)
    mass = dot_across(ones, score_high) + dot_across(ones, score_low) + dot_across(ones, score_last)
    row8 = iota((8, lanes), 0)
    stat_mine[0] = jnp.where(row8 == 0, load, jnp.where(row8 == 1, mass, 0.0))

    spread = (iota((lanes, slots), 0) == (iota((lanes, slots), 1) >> 4)).astype(F32).astype(BF16)
    place = jnp.where(
        dot_down(rank16, spread) == (iota((toks, slots), 1) & 15).astype(F32),
        dot_down(named16, spread),
        0.0,
    ).astype(BF16)

    wide = 128
    slot_wide = (iota((toks, wide), 1) & 15).astype(F32)
    for z in range(ZH):
        pick = (iota((lanes, wide), 0) == expert_of(iota((lanes, wide), 1) >> 4, z)).astype(F32).astype(BF16)
        there = dot_down(rank16, pick) == slot_wide
        w_send[z, 0] = jnp.where(there, dot_down(score_high, pick), 0.0).astype(BF16)
        w_send[z, 1] = jnp.where(there, dot_down(score_low, pick), 0.0).astype(BF16)

    pl.semaphore_wait(barrier, EXPERTS - 1 + GROUPS - 1)

    full = {"g": gate_w, "u": up_w, "d": down_w}
    own = {"g": wg, "u": wu, "d": wd}

    def region(array, z, away, first, count):
        if array == "d":
            group = z * Y + (away + 1) % Y
            return down_w.at[pl.ds(group * piece + first * half, count * half), :]
        group = (zl if z == 0 else 1 - zl) * Y + (y + away + Y) % Y
        return full[array].at[pl.ds(pl.multiple_of(group * piece + first * half, 16), count * half), :]

    order = {RIGHT: ring_messages(RIGHT), LEFT: ring_messages(LEFT)}
    index = {s: {m[:4]: n for n, m in enumerate(order[s])} for s in order}
    side = {RIGHT: 0, LEFT: 1}
    arrived, started, zx_done = set(), [], set()
    zx = {}

    def start_zx(array):
        n = "gud".index(array)
        c = remote(
            own[array], region(array, int(array == "d"), 0, 0, 2), zx_send.at[n], zx_recv.at[n], partner, me
        )
        c.start()
        zx[array] = c

    def wait_zx(array):
        if array not in zx_done:
            zx_done.add(array)
            n = "gud".index(array)
            there = region(array, 1, 0, 0, 2)
            remote(there, there, zx_send.at[n], zx_recv.at[n], partner, me).wait_recv()

    def wait_ring(s, n):
        if (s, n) in arrived:
            return
        arrived.add((s, n))
        array, z, hops, first, count = order[s][n]
        there = region(array, z, -s * (hops + 1), first, count)
        remote(
            there, there, ring_send.at[side[s], n], ring_recv.at[side[s], n], dp, me
        ).wait_recv()

    def forward(s, n):
        array, z, hops, first, count = order[s][n]
        if hops:
            if (array, z, hops - 1, first) in index[s]:
                wait_ring(s, index[s][(array, z, hops - 1, first)])
        elif z:
            wait_zx(array)
        if hops == 0 and z == 0:
            src = own[array].at[pl.ds(first * half, count * half), :]
        else:
            src = region(array, z, -s * hops, first, count)
        if array == "d":
            dst = region(array, z, -s * (hops + 1), first, count)
        else:
            dst = region(array, z, -s * hops, first, count)
        c = remote(
            src,
            dst,
            ring_send.at[side[s], n],
            ring_recv.at[side[s], n],
            zl * Y + (y + s + Y) % Y,
            me,
        )
        c.start()
        started.append(c)

    def ring_step(n):
        forward(RIGHT, n)
        forward(LEFT, n)


    def row_block(ref, n):
        return ref.at[pl.ds(pl.multiple_of(n * CAP, CAP), CAP), :]

    def row_copy(k):
        to = (me + k) % EXPERTS
        return remote(row_block(outgoing, to), row_block(rows, pos), row_send.at[k], row_recv.at[k], dp, to)

    def row_start(k, carry):
        row_copy(k).start()
        return carry

    def row_wait(k, carry):
        source = (me - k + EXPERTS) % EXPERTS
        place_of = ((source // (C * ZH)) * C + source % C) * ZH + (source // C) % ZH
        there = row_block(rows, place_of)
        remote(there, there, row_send.at[k], row_recv.at[k], dp, me).wait_recv()
        return carry

    def row_sent(k, carry):
        row_copy(k).wait_send()
        return carry

    def w_copy(k):
        to = (zh + k) % ZH
        return remote(w_send.at[to], w_recv.at[zh], w_ssem.at[k], w_rsem.at[k], dp, expert_index(x, to, core))

    def stat_a_copy(k):
        to = (dp + k) % GROUPS
        return remote(stat_mine.at[0], stat_a.at[dp], sa_send.at[k], sa_recv.at[k], to, me)

    def stat_b_copy(k):
        to = (me + k) % EXPERTS
        return remote(stat_mine.at[1], stat_b.at[me], sb_send.at[k], sb_recv.at[k], dp, to)

    def starts(copy, count):
        def one(k, carry):
            copy(k).start()
            return carry

        lax.fori_loop(1, count, one, 0)

    def sent(copy, count):
        def one(k, carry):
            copy(k).wait_send()
            return carry

        lax.fori_loop(1, count, one, 0)

    starts(stat_a_copy, GROUPS)
    for k in range(1, ZH):
        w_copy(k).start()
    start_zx("g")
    start_zx("u")
    ring_step(0)
    ring_step(1)

    def send_part(k, carry):
        at = pl.ds(pl.multiple_of(k * 512, 512), 512)
        outgoing[:, at] = lax.dot_general(
            place, tokens[:, at], (((0,), (0,)), ((), ())), preferred_element_type=F32
        ).astype(BF16)
        return carry

    lax.fori_loop(0, width // 512, send_part, 0)

    lax.fori_loop(1, EXPERTS, row_start, 0)
    start_zx("d")
    stat_a[dp] = stat_mine[0]
    w_recv[zh] = w_send[zh]
    mine = pl.ds(pl.multiple_of(dp * piece, 16), piece)
    rows[pl.ds(pl.multiple_of(pos * CAP, CAP), CAP), :] = outgoing[
        pl.ds(pl.multiple_of(me * CAP, CAP), CAP), :
    ]
    gate_w[mine, :] = wg[...]
    up_w[mine, :] = wu[...]
    down_w[pl.ds(piece, piece), :] = wd[...]

    ring_step(2)
    ring_step(3)

    def stat_a_wait(k, carry):
        there = stat_a.at[(dp - k + GROUPS) % GROUPS]
        remote(there, there, sa_send.at[k], sa_recv.at[k], dp, me).wait_recv()
        return carry

    lax.fori_loop(1, GROUPS, stat_a_wait, 0)
    stat_mine[1] = jnp.sum(stat_a[...], axis=0)
    starts(stat_b_copy, EXPERTS)
    stat_b[me] = stat_mine[1]

    def stat_b_wait(k, carry):
        there = stat_b.at[(me - k + EXPERTS) % EXPERTS]
        remote(there, there, sb_send.at[k], sb_recv.at[k], dp, me).wait_recv()
        return carry

    for n in range(4, 8):
        ring_step(n)

    for k in range(1, ZH):
        there = w_recv.at[(zh - k + ZH) % ZH]
        remote(there, there, w_ssem.at[k], w_rsem.at[k], dp, me).wait_recv()
    from_slot, to_slot = iota((wide, slots), 0), iota((wide, slots), 1)
    for z in range(ZH):
        widen = (
            ((to_slot >> 6) == (from_slot >> 4))
            & (((to_slot >> 4) & 3) == z)
            & ((to_slot & 15) == (from_slot & 15))
        )
        widen = widen.astype(F32).astype(BF16)
        for part in range(2):
            w_wide[pl.ds((part * ZH + z) * toks, toks), :] = dot(w_recv[z, part], widen).astype(BF16)

    for n in range(8, 18):
        ring_step(n)

    lax.fori_loop(1, EXPERTS, row_wait, 0)
    for s in (RIGHT, LEFT):
        for n in range(GATE_UP):
            wait_ring(s, n)

    part_width = 256
    block = slots // 2
    for n in range(hid // part_width):
        columns = slice(n * part_width, (n + 1) * part_width)

        def hidden_rows(m, carry, columns=columns):
            at = pl.ds(pl.multiple_of(m * block, block), block)
            gate = dot(rows[at, :], gate_w[:, columns])
            up = dot(rows[at, :], up_w[:, columns])
            hidden[at, columns] = (gate / (1.0 + jnp.exp(-gate)) * up).astype(BF16)
            return carry

        lax.fori_loop(0, slots // block, hidden_rows, 0)
        if n:
            ring_step(17 + n)

    def block_of(ref, at):
        return ref.at[pl.ds(pl.multiple_of(at * ZH * CAP, ZH * CAP), ZH * CAP), :]

    def x_copy(n):
        def copy(k):
            to = (xc + k) % XC
            return remote(
                block_of(produced[n], to),
                block_of(x_in[n], xc),
                xp_send.at[n, k],
                xp_recv.at[n, k],
                dp,
                expert_index(to // C, zh, to % C),
            )

        return copy

    def z_copy(n):
        def copy(k):
            to = (zh + k) % ZH
            return remote(
                partial[n].at[to],
                z_in[n].at[zh],
                zp_send.at[n, k],
                zp_recv.at[n, k],
                dp,
                expert_index(x, to, core),
            )

        return copy

    def wait_down(z, first, columns):
        needed = range(first // piece, -(-(first + columns) // piece))
        for s in (RIGHT, LEFT):
            for m in range(GATE_UP, MESSAGES):
                if order[s][m][1] == z and (1 - s * (order[s][m][2] + 1)) % Y in needed:
                    wait_ring(s, m)

    def produce(n):
        z, first, columns = CHUNKS[n]
        wait_down(z, first, columns)
        produced[n][...] = dot_across(
            hidden[...], down_w[pl.ds(z * Y * piece + first, columns), :]
        ).astype(BF16)
        starts(x_copy(n), XC)
        at = pl.ds(pl.multiple_of(xc * ZH * CAP, ZH * CAP), ZH * CAP)
        x_in[n][at, :] = produced[n][at, :]

    def combine(n):
        def wait(k, carry):
            there = block_of(x_in[n], (xc - k + XC) % XC)
            remote(there, there, xp_send.at[n, k], xp_recv.at[n, k], dp, me).wait_recv()
            return carry

        lax.fori_loop(1, XC, wait, 0)
        both = dot(w_wide[...], x_in[n][...])
        summed = (both[: ZH * toks] + both[ZH * toks :]).astype(BF16)
        for z in range(ZH):
            partial[n][z] = summed[z * toks : (z + 1) * toks]
        starts(z_copy(n), ZH)
        z_in[n][zh] = partial[n][zh]

    def finish(n):
        def wait(k, carry):
            there = z_in[n].at[(zh - k + ZH) % ZH]
            remote(there, there, zp_send.at[n, k], zp_recv.at[n, k], dp, me).wait_recv()
            return carry

        lax.fori_loop(1, ZH, wait, 0)
        result = z_in[n][0].astype(F32)
        for z in range(1, ZH):
            result = result + z_in[n][z].astype(F32)
        z, first, columns = CHUNKS[n]
        relative[z, :, first : first + columns] = result

    def place_columns(z):
        there = pl.multiple_of((zl if z == 0 else 1 - zl) * Y * piece, Y * piece)
        turned = pltpu.roll(relative[z], ((y + Y - 1) % Y) * piece, 1)
        out[:, pl.ds(there, Y * piece)] = turned.astype(BF16)

    produce(0)
    ring_step(20)
    ring_step(21)
    produce(1)
    ring_step(22)
    ring_step(23)
    produce(2)
    combine(0)
    ring_step(24)
    produce(3)
    combine(1)
    ring_step(25)
    ring_step(26)
    produce(4)
    combine(2)
    finish(0)
    ring_step(27)
    produce(5)
    combine(3)
    finish(1)
    produce(6)
    combine(4)
    finish(2)
    produce(7)
    produce(8)

    lax.fori_loop(1, EXPERTS, stat_b_wait, 0)
    totals = jnp.sum(stat_b[...], axis=0)
    count, masses = totals[0:1, :], totals[1:2, :]
    total = toks * GROUPS * EXPERTS
    loss = jnp.sum(
        (EXPERTS * count / (topk * total)) * (masses / total), axis=1, keepdims=True
    )
    my_load = jnp.sum(jnp.where(iota((1, lanes), 1) == me, count, 0.0), axis=1, keepdims=True)
    stat_out[...] = jnp.where(row8 == 0, my_load, jnp.where(row8 == 1, loss, 0.0))

    finish(3)
    combine(5)
    finish(4)
    combine(6)
    combine(7)
    combine(8)
    finish(5)
    place_columns(0)
    finish(6)
    finish(7)
    finish(8)
    place_columns(1)

    for c in started:
        c.wait_send()
    for array in "gud":
        zx[array].wait_send()
    for k in range(1, ZH):
        w_copy(k).wait_send()
    lax.fori_loop(1, EXPERTS, row_sent, 0)
    sent(stat_a_copy, GROUPS)
    sent(stat_b_copy, EXPERTS)
    for n in range(len(CHUNKS)):
        sent(x_copy(n), XC)
        sent(z_copy(n), ZH)


def on_device(tokens, expert_ids, gate_scores, w_gate, w_up, w_down):
    toks, width = tokens.shape
    hid = w_gate.shape[2]
    slots = EXPERTS * CAP
    dma = pltpu.SemaphoreType.DMA
    vmem = pl.BlockSpec(memory_space=pltpu.VMEM)
    mixed, stats = pl.pallas_call(
        kernel,
        out_shape=(
            jax.ShapeDtypeStruct((toks, width), BF16),
            jax.ShapeDtypeStruct((8, 128), F32),
        ),
        in_specs=[vmem] * 6,
        out_specs=(vmem, vmem),
        scratch_shapes=[
            pltpu.VMEM((width, hid), BF16),
            pltpu.VMEM((width, hid), BF16),
            pltpu.VMEM((width, hid), BF16),
            pltpu.VMEM((slots, width), BF16),
            pltpu.VMEM((slots, width), BF16),
            pltpu.VMEM((slots, hid), BF16),
            pltpu.VMEM((ZL, toks, width // ZL), F32),
            pltpu.VMEM((ZH, 2, toks, 128), BF16),
            pltpu.VMEM((ZH, 2, toks, 128), BF16),
            pltpu.VMEM((2 * ZH * toks, slots), BF16),
            pltpu.VMEM((GROUPS, 8, 128), F32),
            pltpu.VMEM((EXPERTS, 8, 128), F32),
            pltpu.VMEM((2, 8, 128), F32),
            dma((2, MESSAGES)),
            dma((2, MESSAGES)),
            dma((3,)),
            dma((3,)),
            dma((EXPERTS,)),
            dma((EXPERTS,)),
            dma((ZH,)),
            dma((ZH,)),
            dma((GROUPS,)),
            dma((GROUPS,)),
            dma((EXPERTS,)),
            dma((EXPERTS,)),
            dma((len(CHUNKS), XC)),
            dma((len(CHUNKS), XC)),
            dma((len(CHUNKS), ZH)),
            dma((len(CHUNKS), ZH)),
        ]
        + [pltpu.VMEM((slots, w), BF16) for _, _, w in CHUNKS] * 2
        + [pltpu.VMEM((ZH, toks, w), BF16) for _, _, w in CHUNKS] * 2,
        compiler_params=pltpu.CompilerParams(
            collective_id=0, has_side_effects=True, vmem_limit_bytes=60 * 1024 * 1024
        ),
        name="routed_layer",
    )(tokens, expert_ids.T, gate_scores.T, w_gate[0], w_up[0], w_down[0].T)
    return mixed, stats[0, :1].astype(I32), stats[1, 0]


def solution(mesh):
    both = ("dp", "expert")
    return jax.shard_map(
        on_device,
        mesh=mesh,
        in_specs=(
            P(both, None),
            P(both, None),
            P(both, None),
            P("expert", "dp", None),
            P("expert", "dp", None),
            P("expert", None, "dp"),
        ),
        out_specs=(P(both, None), P("expert"), P()),
        check_vma=False,
    )
```

```python
import functools

import jax
import jax.numpy as jnp
from jax import lax
from jax.experimental import pallas as pl
from jax.experimental.pallas import tpu as pltpu
from jax.sharding import PartitionSpec as P

F32, BF16, I32 = jnp.float32, jnp.bfloat16, jnp.int32
X, ZH, C, ZL, Y = 4, 4, 2, 2, 8
CAP = 16
XC = X * C
EXPERTS = X * ZH * C
GROUPS = ZL * Y
RIGHT, LEFT = 1, -1
CHUNKS = (
    (0, 0, 384),
    (1, 0, 384),
    (0, 384, 256),
    (0, 1024, 256),
    (0, 640, 384),
    (1, 384, 256),
    (1, 1024, 256),
    (1, 640, 256),
    (1, 896, 128),
)


def iota(shape, dim):
    return lax.broadcasted_iota(I32, shape, dim)


def dot(a, b):
    return jnp.dot(a, b, preferred_element_type=F32)


def dot_down(a, b):
    return lax.dot_general(a, b, (((0,), (0,)), ((), ())), preferred_element_type=F32)


def dot_across(a, b):
    return lax.dot_general(a, b, (((1,), (1,)), ((), ())), preferred_element_type=F32)


def remote(src, dst, send, recv, dp, ex):
    return pltpu.make_async_remote_copy(
        src_ref=src,
        dst_ref=dst,
        send_sem=send,
        recv_sem=recv,
        device_id=(dp, ex),
        device_id_type=pl.DeviceIdType.MESH,
    )


def expert_of(xc, zh):
    return ((xc >> 1) * ZH + zh) * C + (xc & 1)


def expert_index(x, zh, core):
    return (x * ZH + zh) * C + core


def ring_messages(direction):
    far = "g" if direction == RIGHT else "u"
    half = 0 if direction == RIGHT else 1
    out = []
    near = "u" if direction == RIGHT else "g"
    for hops in range(3):
        out += [("g", 0, hops, 0, 2), ("u", 0, hops, 0, 2)]
    out.append((far, 0, 3, 0, 2))
    for hops in range(2):
        out += [("g", 1, hops, 0, 2), ("u", 1, hops, 0, 2)]
    out.append((near, 1, 2, 0, 2))
    for z, hops, first in (
        [(0, 0, half), (0, 0, 1 - half), (1, 0, half), (1, 0, 1 - half), (0, 1, half), (0, 1, 1 - half)]
        + [(0, 2, half), (1, 1, half), (0, 2, 1 - half), (0, 3, half), (1, 1, 1 - half)]
        + [(1, 2, half), (1, 2, 1 - half), (1, 3, half)]
    ):
        out.append(("d", z, hops, first, 1))
    return out


MESSAGES = len(ring_messages(RIGHT))
GATE_UP = 12
SHARED = (("g", -3, RIGHT, 4), ("u", 3, LEFT, 5), ("g", -4, RIGHT, 6), ("u", 4, LEFT, 6))
PARTS = 2


def kernel(
    tokens,
    ids_in,
    scores_in,
    wg,
    wu,
    wd,
    out,
    load_out,
    loss_out,
    ids,
    scores,
    gate_w,
    up_w,
    down_w,
    hidden,
    relative,
    w_send,
    w_recv,
    w_wide,
    stat_a,
    stat_b,
    stat_mine,
    load_sem,
    ring_send,
    ring_recv,
    zx_send,
    zx_recv,
    share_send,
    share_recv,
    token_send,
    token_recv,
    row_send,
    row_recv,
    w_ssem,
    w_rsem,
    sa_send,
    sa_recv,
    sb_send,
    sb_recv,
    xp_send,
    xp_recv,
    zp_send,
    zp_recv,
    *buffers,
):
    (token_part, token_all, outgoing, rows), chunk_buffers = (
        [buffers[n * PARTS : (n + 1) * PARTS] for n in range(4)],
        buffers[4 * PARTS :],
    )
    produced, x_in, partial, z_in = (
        chunk_buffers[n * len(CHUNKS) : (n + 1) * len(CHUNKS)] for n in range(4)
    )
    toks, width = tokens.shape
    piece, hid = wg.shape
    half = piece // 2
    slots = EXPERTS * CAP
    topk = ids.shape[0]

    dp = lax.axis_index("dp")
    me = lax.axis_index("expert")
    zl, y = dp // Y, dp % Y
    core, zh, x = me % C, (me // C) % ZH, me // (C * ZH)
    xc = x * C + core
    partner = (1 - zl) * Y + y

    part = width // PARTS
    mine = pl.ds(pl.multiple_of(dp * piece, 16), piece)
    loads = [
        pltpu.make_async_copy(source, target, load_sem.at[n])
        for n, (source, target) in enumerate(
            [(ids_in, ids), (scores_in, scores)]
            + [(wg, gate_w.at[mine, :]), (wu, up_w.at[mine, :]), (wd, down_w.at[pl.ds(piece, piece), :])]
            + [(tokens.at[:, n * part : (n + 1) * part], token_part[n]) for n in range(PARTS)]
        )
    ]
    for c in loads:
        c.start()

    barrier = pltpu.get_barrier_semaphore()

    def greet_expert(k, carry):
        pl.semaphore_signal(
            barrier, inc=1, device_id=(dp, (me + k) % EXPERTS), device_id_type=pl.DeviceIdType.MESH
        )
        return carry

    def greet_group(k, carry):
        pl.semaphore_signal(
            barrier, inc=1, device_id=((dp + k) % GROUPS, me), device_id_type=pl.DeviceIdType.MESH
        )
        return carry

    lax.fori_loop(1, GROUPS, greet_group, 0)
    lax.fori_loop(1, EXPERTS, greet_expert, 0)

    for c in loads[2:5]:
        c.wait()

    pl.semaphore_wait(barrier, EXPERTS - 1 + GROUPS - 1)

    def all_of(ref, send, recv):
        return remote(ref, ref, send, recv, dp, me)

    full = {"g": gate_w, "u": up_w, "d": down_w}

    def region(array, z, away, first, count):
        if array == "d":
            group = z * Y + (away + 1) % Y
            return down_w.at[pl.ds(group * piece + first * half, count * half), :]
        group = (zl if z == 0 else 1 - zl) * Y + (y + away + Y) % Y
        return full[array].at[pl.ds(pl.multiple_of(group * piece + first * half, 16), count * half), :]

    order = {RIGHT: ring_messages(RIGHT), LEFT: ring_messages(LEFT)}
    index = {s: {m[:4]: n for n, m in enumerate(order[s])} for s in order}
    side = {RIGHT: 0, LEFT: 1}
    arrived, zx_done = set(), set()

    def start_zx(array):
        n = "gud".index(array)
        c = remote(
            region(array, 0, 0, 0, 2),
            region(array, int(array == "d"), 0, 0, 2),
            zx_send.at[0],
            zx_recv.at[n],
            partner,
            me,
        )
        c.start()

    def wait_zx(array):
        if array not in zx_done:
            zx_done.add(array)
            n = "gud".index(array)
            there = region(array, 1, 0, 0, 2)
            remote(there, there, zx_send.at[0], zx_recv.at[n], partner, me).wait_recv()

    def wait_ring(s, n):
        if (s, n) in arrived:
            return
        arrived.add((s, n))
        array, z, hops, first, count = order[s][n]
        there = region(array, z, -s * (hops + 1), first, count)
        remote(there, there, ring_send.at[side[s], 0], ring_recv.at[side[s], n], dp, me).wait_recv()

    def forward(s, n):
        array, z, hops, first, count = order[s][n]
        if hops:
            if (array, z, hops - 1, first) in index[s]:
                wait_ring(s, index[s][(array, z, hops - 1, first)])
        elif z:
            wait_zx(array)
        src = region(array, z, -s * hops, first, count)
        if array == "d":
            dst = region(array, z, -s * (hops + 1), first, count)
        else:
            dst = region(array, z, -s * hops, first, count)
        c = remote(
            src,
            dst,
            ring_send.at[side[s], int(n >= GATE_UP)],
            ring_recv.at[side[s], n],
            zl * Y + (y + s + Y) % Y,
            me,
        )
        c.start()

    def ring_step(n):
        forward(RIGHT, n)
        forward(LEFT, n)


    def block_of(ref, at):
        return ref.at[pl.ds(pl.multiple_of(at * ZH * CAP, ZH * CAP), ZH * CAP), :]

    def token_copy(n):
        def copy(k):
            to = (zh + k) % ZH
            return remote(
                token_part[n],
                block_of(token_all[n], zh),
                token_send.at[n],
                token_recv.at[n],
                dp,
                expert_index(x, to, core),
            )

        return copy

    def row_copy(n):
        def copy(k):
            to = (xc + k) % XC
            return remote(
                block_of(outgoing[n], to),
                block_of(rows[n], xc),
                row_send.at[n],
                row_recv.at[n],
                dp,
                expert_index(to // C, zh, to % C),
            )

        return copy

    def gather_send(n):
        starts(token_copy(n), ZH)
        token_all[n][pl.ds(pl.multiple_of(zh * toks, toks), toks), :] = token_part[n][...]

    def rows_send(n):
        all_of(token_all[n].at[: (ZH - 1) * toks], token_send.at[n], token_recv.at[n]).wait_recv()
        step = 256

        def some(m, carry):
            at = pl.ds(pl.multiple_of(m * step, step), step)
            outgoing[n][:, at] = dot_down(
                w_wide[2 * ZH * toks :, :], token_all[n][:, at]
            ).astype(BF16)
            return carry

        lax.fori_loop(0, part // step, some, 0)
        starts(row_copy(n), XC)
        at = pl.ds(pl.multiple_of(xc * ZH * CAP, ZH * CAP), ZH * CAP)
        rows[n][at, :] = outgoing[n][at, :]

    def rows_take(n):
        all_of(rows[n].at[: (XC - 1) * ZH * CAP], row_send.at[n], row_recv.at[n]).wait_recv()

    def share(n):
        array, away, s, m = SHARED[n]
        wait_ring(s, m)
        c = remote(
            region(array, 0, away, 0, 2),
            region(array, 0, away, 0, 2),
            share_send.at[0],
            share_recv.at[n],
            partner,
            me,
        )
        c.start()

    def wait_share(n):
        array, away, _, _ = SHARED[n]
        there = region(array, 1, away, 0, 2)
        remote(there, there, share_send.at[0], share_recv.at[n], partner, me).wait_recv()

    def w_copy(k):
        to = (zh + k) % ZH
        return remote(w_send.at[to], w_recv.at[zh], w_ssem.at[0], w_rsem.at[0], dp, expert_index(x, to, core))

    def stat_a_copy(k):
        to = (dp + k) % GROUPS
        return remote(stat_mine.at[0], stat_a.at[dp], sa_send.at[0], sa_recv.at[0], to, me)

    def stat_b_copy(k):
        to = (me + k) % EXPERTS
        return remote(stat_mine.at[1], stat_b.at[me], sb_send.at[0], sb_recv.at[0], dp, to)

    def starts(copy, count):
        def one(k, carry):
            copy(k).start()
            return carry

        lax.fori_loop(1, count, one, 0)

    ring_step(0)
    ring_step(1)

    loads[0].wait()
    loads[1].wait()

    lanes = 128
    expert_row = iota((lanes, toks), 0)
    named = jnp.zeros((lanes, toks), F32)
    score = jnp.zeros((lanes, toks), F32)
    for k in range(topk):
        hit = ids[k : k + 1, :] == expert_row
        named = named + jnp.where(hit, 1.0, 0.0)
        score = score + jnp.where(hit, scores[k : k + 1, :], 0.0)
    earlier = (iota((toks, toks), 0) < iota((toks, toks), 1)).astype(F32).astype(BF16)
    named16 = named.astype(BF16)
    rank16 = dot(named16, earlier).astype(BF16)
    score_high = score.astype(BF16)
    rest = score - score_high.astype(F32)
    score_low = rest.astype(BF16)
    score_last = (rest - score_low.astype(F32)).astype(BF16)

    ones = jnp.ones((8, toks), BF16)
    load = dot_across(ones, named16)
    mass = dot_across(ones, score_high) + dot_across(ones, score_low) + dot_across(ones, score_last)
    row8 = iota((8, lanes), 0)
    stat_mine[0] = jnp.where(row8 == 0, load, jnp.where(row8 == 1, mass, 0.0))

    wide = 128
    slot_wide = (iota((toks, wide), 1) & 15).astype(F32)
    for z in range(ZH):
        pick = (iota((lanes, wide), 0) == expert_of(iota((lanes, wide), 1) >> 4, z)).astype(F32).astype(BF16)
        there = dot_down(rank16, pick) == slot_wide
        w_send[z, 0] = jnp.where(there, dot_down(score_high, pick), 0.0).astype(BF16)
        w_send[z, 1] = jnp.where(there, dot_down(score_low, pick), 0.0).astype(BF16)
        w_send[z, 2] = jnp.where(there, dot_down(named16, pick), 0.0).astype(BF16)

    starts(stat_a_copy, GROUPS)
    for k in range(1, ZH):
        w_copy(k).start()
    loads[5].wait()
    gather_send(0)
    start_zx("g")
    loads[6].wait()
    gather_send(1)
    start_zx("u")
    start_zx("d")
    stat_a[dp] = stat_mine[0]
    w_recv[zh] = w_send[zh]

    ring_step(2)
    ring_step(3)

    all_of(w_recv.at[: ZH - 1], w_ssem.at[0], w_rsem.at[0]).wait_recv()
    from_slot, to_slot = iota((wide, slots), 0), iota((wide, slots), 1)
    for z in range(ZH):
        widen = (
            ((to_slot >> 6) == (from_slot >> 4))
            & (((to_slot >> 4) & 3) == z)
            & ((to_slot & 15) == (from_slot & 15))
        )
        widen = widen.astype(F32).astype(BF16)
        for kind in range(3):
            w_wide[pl.ds((kind * ZH + z) * toks, toks), :] = dot(w_recv[z, kind], widen).astype(BF16)

    for n in range(4, 7):
        ring_step(n)
    rows_send(0)
    ring_step(7)
    ring_step(8)
    share(0)
    share(1)
    rows_send(1)
    share(2)
    share(3)

    all_of(stat_a.at[: GROUPS - 1], sa_send.at[0], sa_recv.at[0]).wait_recv()
    stat_mine[1] = jnp.sum(stat_a[...], axis=0)
    starts(stat_b_copy, EXPERTS)
    stat_b[me] = stat_mine[1]

    for n in range(9, GATE_UP + 4):
        ring_step(n)

    rows_take(0)
    rows_take(1)
    for n in range(len(SHARED)):
        wait_share(n)
    for s in (RIGHT, LEFT):
        for n in range(GATE_UP):
            wait_ring(s, n)

    part_width = 256
    block = slots // 2
    for n in range(hid // part_width):
        columns = slice(n * part_width, (n + 1) * part_width)

        def hidden_rows(m, carry, columns=columns):
            at = pl.ds(pl.multiple_of(m * block, block), block)
            gate = sum(
                dot(rows[k][at, :], gate_w[k * part : (k + 1) * part, columns]) for k in range(PARTS)
            )
            up = sum(
                dot(rows[k][at, :], up_w[k * part : (k + 1) * part, columns]) for k in range(PARTS)
            )
            hidden[at, columns] = (gate / (1.0 + jnp.exp(-gate)) * up).astype(BF16)
            return carry

        lax.fori_loop(0, slots // block, hidden_rows, 0)
        if n:
            ring_step(GATE_UP + 3 + n)

    def x_copy(n):
        def copy(k):
            to = (xc + k) % XC
            return remote(
                block_of(produced[n], to),
                block_of(x_in[n], xc),
                xp_send.at[n],
                xp_recv.at[n],
                dp,
                expert_index(to // C, zh, to % C),
            )

        return copy

    def z_copy(n):
        def copy(k):
            to = (zh + k) % ZH
            return remote(
                partial[n].at[to],
                z_in[n].at[zh],
                zp_send.at[n],
                zp_recv.at[n],
                dp,
                expert_index(x, to, core),
            )

        return copy

    def wait_down(z, first, columns):
        needed = range(first // piece, -(-(first + columns) // piece))
        for s in (RIGHT, LEFT):
            for m in range(GATE_UP, MESSAGES):
                if order[s][m][1] == z and (1 - s * (order[s][m][2] + 1)) % Y in needed:
                    wait_ring(s, m)

    def produce(n):
        z, first, columns = CHUNKS[n]
        wait_down(z, first, columns)
        produced[n][...] = dot_across(
            hidden[...], down_w[pl.ds(z * Y * piece + first, columns), :]
        ).astype(BF16)
        starts(x_copy(n), XC)
        at = pl.ds(pl.multiple_of(xc * ZH * CAP, ZH * CAP), ZH * CAP)
        x_in[n][at, :] = produced[n][at, :]

    def combine(n):
        all_of(x_in[n].at[: (XC - 1) * ZH * CAP], xp_send.at[n], xp_recv.at[n]).wait_recv()
        both = dot(w_wide[: 2 * ZH * toks, :], x_in[n][...])
        summed = (both[: ZH * toks] + both[ZH * toks :]).astype(BF16)
        for z in range(ZH):
            partial[n][z] = summed[z * toks : (z + 1) * toks]
        starts(z_copy(n), ZH)
        z_in[n][zh] = partial[n][zh]

    def finish(n):
        all_of(z_in[n].at[: ZH - 1], zp_send.at[n], zp_recv.at[n]).wait_recv()
        result = z_in[n][0].astype(F32)
        for z in range(1, ZH):
            result = result + z_in[n][z].astype(F32)
        z, first, columns = CHUNKS[n]
        relative[z, :, first : first + columns] = result

    def place_columns(z):
        there = pl.multiple_of((zl if z == 0 else 1 - zl) * Y * piece, Y * piece)
        turned = pltpu.roll(relative[z], ((y + Y - 1) % Y) * piece, 1)
        out[:, pl.ds(there, Y * piece)] = turned.astype(BF16)

    produce(0)
    produce(1)
    ring_step(GATE_UP + 6)
    ring_step(GATE_UP + 7)
    ring_step(GATE_UP + 8)
    produce(2)
    combine(0)
    ring_step(GATE_UP + 9)
    ring_step(GATE_UP + 10)
    combine(1)
    ring_step(GATE_UP + 11)
    produce(3)
    combine(2)
    finish(0)
    produce(4)
    ring_step(GATE_UP + 12)
    produce(5)
    combine(3)
    finish(1)
    ring_step(GATE_UP + 13)
    all_of(stat_b.at[: EXPERTS - 1], sb_send.at[0], sb_recv.at[0]).wait_recv()
    totals = jnp.sum(stat_b[...], axis=0)
    count, masses = totals[0:1, :], totals[1:2, :]
    total = toks * GROUPS * EXPERTS
    loss = jnp.sum(
        (EXPERTS * count / (topk * total)) * (masses / total), axis=1, keepdims=True
    )
    my_load = jnp.sum(jnp.where(iota((1, lanes), 1) == me, count, 0.0), axis=1, keepdims=True)
    load_out[...] = my_load.astype(I32)
    loss_out[...] = loss

    finish(2)
    produce(6)
    combine(4)
    finish(3)
    produce(7)
    produce(8)
    combine(5)
    combine(6)
    finish(4)
    place_columns(0)
    combine(7)
    combine(8)
    for n in range(5, len(CHUNKS)):
        finish(n)
    place_columns(1)

    for s in (0, 1):
        all_of(gate_w.at[: GATE_UP * piece], ring_send.at[s, 0], ring_recv.at[s, 0]).wait_send()
        all_of(
            down_w.at[: (MESSAGES - GATE_UP) * half], ring_send.at[s, 1], ring_recv.at[s, 0]
        ).wait_send()
    all_of(gate_w.at[: 3 * piece], zx_send.at[0], zx_recv.at[0]).wait_send()
    all_of(gate_w.at[: len(SHARED) * piece], share_send.at[0], share_recv.at[0]).wait_send()
    all_of(w_recv.at[: ZH - 1], w_ssem.at[0], w_rsem.at[0]).wait_send()
    all_of(stat_a.at[: GROUPS - 1], sa_send.at[0], sa_recv.at[0]).wait_send()
    all_of(stat_b.at[: EXPERTS - 1], sb_send.at[0], sb_recv.at[0]).wait_send()
    for n in range(PARTS):
        all_of(token_all[n].at[: (ZH - 1) * toks], token_send.at[n], token_recv.at[n]).wait_send()
        all_of(rows[n].at[: (XC - 1) * ZH * CAP], row_send.at[n], row_recv.at[n]).wait_send()
    for n in range(len(CHUNKS)):
        all_of(x_in[n].at[: (XC - 1) * ZH * CAP], xp_send.at[n], xp_recv.at[n]).wait_send()
        all_of(z_in[n].at[: ZH - 1], zp_send.at[n], zp_recv.at[n]).wait_send()


def on_device(tokens, expert_ids, gate_scores, w_gate, w_up, w_down):
    toks, width = tokens.shape
    hid = w_gate.shape[2]
    slots = EXPERTS * CAP
    dma = pltpu.SemaphoreType.DMA
    vmem = pl.BlockSpec(memory_space=pltpu.VMEM)
    mixed, load, loss = pl.pallas_call(
        kernel,
        out_shape=(
            jax.ShapeDtypeStruct((toks, width), BF16),
            jax.ShapeDtypeStruct((1, 1), I32),
            jax.ShapeDtypeStruct((1, 1), F32),
        ),
        in_specs=[pl.BlockSpec(memory_space=pl.ANY)] * 6,
        out_specs=(vmem, vmem, vmem),
        scratch_shapes=[
            pltpu.VMEM(expert_ids.shape[::-1], I32),
            pltpu.VMEM(expert_ids.shape[::-1], F32),
            pltpu.VMEM((width, hid), BF16),
            pltpu.VMEM((width, hid), BF16),
            pltpu.VMEM((width, hid), BF16),
            pltpu.VMEM((slots, hid), BF16),
            pltpu.VMEM((ZL, toks, width // ZL), F32),
            pltpu.VMEM((ZH, 3, toks, 128), BF16),
            pltpu.VMEM((ZH, 3, toks, 128), BF16),
            pltpu.VMEM((3 * ZH * toks, slots), BF16),
            pltpu.VMEM((GROUPS, 8, 128), F32),
            pltpu.VMEM((EXPERTS, 8, 128), F32),
            pltpu.VMEM((2, 8, 128), F32),
            dma((7,)),
            dma((2, 2)),
            dma((2, MESSAGES)),
            dma((1,)),
            dma((3,)),
            dma((1,)),
            dma((len(SHARED),)),
            dma((PARTS,)),
            dma((PARTS,)),
            dma((PARTS,)),
            dma((PARTS,)),
            dma((1,)),
            dma((1,)),
            dma((1,)),
            dma((1,)),
            dma((1,)),
            dma((1,)),
            dma((len(CHUNKS),)),
            dma((len(CHUNKS),)),
            dma((len(CHUNKS),)),
            dma((len(CHUNKS),)),
        ]
        + [pltpu.VMEM((toks, width // PARTS), BF16)] * PARTS
        + [pltpu.VMEM((ZH * toks, width // PARTS), BF16)] * PARTS
        + [pltpu.VMEM((slots, width // PARTS), BF16)] * (2 * PARTS)
        + [pltpu.VMEM((slots, w), BF16) for _, _, w in CHUNKS] * 2
        + [pltpu.VMEM((ZH, toks, w), BF16) for _, _, w in CHUNKS] * 2,
        compiler_params=pltpu.CompilerParams(
            collective_id=0, has_side_effects=True, vmem_limit_bytes=60 * 1024 * 1024
        ),
        name="routed_layer",
    )(tokens, expert_ids.T, gate_scores.T, w_gate[0], w_up[0], w_down[0].T)
    return mixed, load[0], loss[0, 0]


def solution(mesh):
    both = ("dp", "expert")
    return jax.shard_map(
        on_device,
        mesh=mesh,
        in_specs=(
            P(both, None),
            P(both, None),
            P(both, None),
            P("expert", "dp", None),
            P("expert", "dp", None),
            P("expert", None, "dp"),
        ),
        out_specs=(P(both, None), P("expert"), P()),
        check_vma=False,
    )
```

```python
import functools

import jax
import jax.numpy as jnp
from jax import lax
from jax.experimental import pallas as pl
from jax.experimental.pallas import tpu as pltpu
from jax.sharding import PartitionSpec as P

F32, BF16, I32 = jnp.float32, jnp.bfloat16, jnp.int32
X, ZH, C, ZL, Y = 4, 4, 2, 2, 8
CAP = 16
XC = X * C
EXPERTS = X * ZH * C
GROUPS = ZL * Y
RIGHT, LEFT = 1, -1
CHUNKS = (
    (0, 0, 384),
    (1, 0, 384),
    (0, 384, 256),
    (0, 1024, 256),
    (0, 640, 384),
    (1, 384, 256),
    (1, 1024, 256),
    (1, 640, 256),
    (1, 896, 128),
)


def iota(shape, dim):
    return lax.broadcasted_iota(I32, shape, dim)


def dot(a, b):
    return jnp.dot(a, b, preferred_element_type=F32)


def dot_down(a, b):
    return lax.dot_general(a, b, (((0,), (0,)), ((), ())), preferred_element_type=F32)


def dot_across(a, b):
    return lax.dot_general(a, b, (((1,), (1,)), ((), ())), preferred_element_type=F32)


def remote(src, dst, send, recv, dp, ex):
    return pltpu.make_async_remote_copy(
        src_ref=src,
        dst_ref=dst,
        send_sem=send,
        recv_sem=recv,
        device_id=(dp, ex),
        device_id_type=pl.DeviceIdType.MESH,
    )


def expert_of(xc, zh):
    return ((xc >> 1) * ZH + zh) * C + (xc & 1)


def expert_index(x, zh, core):
    return (x * ZH + zh) * C + core


def ring_messages(direction):
    far = "g" if direction == RIGHT else "u"
    half = 0 if direction == RIGHT else 1
    out = []
    near = "u" if direction == RIGHT else "g"
    for hops in range(3):
        out += [(far, 0, hops, 0, 2), (near, 0, hops, 0, 2)]
    out.append((far, 0, 3, 0, 2))
    for hops in range(2):
        out += [(near, 1, hops, 0, 2), (far, 1, hops, 0, 2)]
    out.append((near, 1, 2, 0, 2))
    for z, hops, first in (
        [(0, 0, half), (0, 0, 1 - half), (1, 0, half), (1, 0, 1 - half), (0, 1, half), (0, 1, 1 - half)]
        + [(1, 1, half), (0, 2, half), (1, 1, 1 - half), (0, 2, 1 - half), (0, 3, half)]
        + [(1, 2, half), (1, 2, 1 - half), (1, 3, half)]
    ):
        out.append(("d", z, hops, first, 1))
    return out


MESSAGES = len(ring_messages(RIGHT))
GATE_UP = 12
SHARED = (("g", -3, RIGHT, 4), ("u", 3, LEFT, 4), ("g", -4, RIGHT, 6), ("u", 4, LEFT, 6))
PARTS = 2


def kernel(
    tokens,
    ids_in,
    scores_in,
    wg,
    wu,
    wd,
    out,
    load_out,
    loss_out,
    ids,
    scores,
    gate_w,
    up_w,
    down_w,
    hidden,
    relative,
    w_send,
    w_recv,
    w_wide,
    stat_a,
    stat_b,
    stat_mine,
    load_sem,
    ring_send,
    ring_recv,
    zx_send,
    zx_recv,
    share_send,
    share_recv,
    token_send,
    token_recv,
    row_send,
    row_recv,
    w_ssem,
    w_rsem,
    sa_send,
    sa_recv,
    sb_send,
    sb_recv,
    xp_send,
    xp_recv,
    zp_send,
    zp_recv,
    *buffers,
):
    (token_part, token_all, outgoing, rows), chunk_buffers = (
        [buffers[n * PARTS : (n + 1) * PARTS] for n in range(4)],
        buffers[4 * PARTS :],
    )
    produced, x_in, partial, z_in = (
        chunk_buffers[n * len(CHUNKS) : (n + 1) * len(CHUNKS)] for n in range(4)
    )
    toks, width = tokens.shape
    piece, hid = wg.shape
    half = piece // 2
    slots = EXPERTS * CAP
    topk = ids.shape[0]

    dp = lax.axis_index("dp")
    me = lax.axis_index("expert")
    zl, y = dp // Y, dp % Y
    core, zh, x = me % C, (me // C) % ZH, me // (C * ZH)
    xc = x * C + core
    partner = (1 - zl) * Y + y

    part = width // PARTS
    mine = pl.ds(pl.multiple_of(dp * piece, 16), piece)
    loads = [
        pltpu.make_async_copy(source, target, load_sem.at[n])
        for n, (source, target) in enumerate(
            [(ids_in, ids), (scores_in, scores)]
            + [(wg, gate_w.at[mine, :]), (wu, up_w.at[mine, :]), (wd, down_w.at[pl.ds(piece, piece), :])]
            + [(tokens.at[:, n * part : (n + 1) * part], token_part[n]) for n in range(PARTS)]
        )
    ]
    for c in loads:
        c.start()

    barrier = pltpu.get_barrier_semaphore()

    def greet_expert(k, carry):
        pl.semaphore_signal(
            barrier, inc=1, device_id=(dp, (me + k) % EXPERTS), device_id_type=pl.DeviceIdType.MESH
        )
        return carry

    def greet_group(k, carry):
        pl.semaphore_signal(
            barrier, inc=1, device_id=((dp + k) % GROUPS, me), device_id_type=pl.DeviceIdType.MESH
        )
        return carry

    lax.fori_loop(1, GROUPS, greet_group, 0)
    lax.fori_loop(1, EXPERTS, greet_expert, 0)

    for c in loads[2:5]:
        c.wait()

    pl.semaphore_wait(barrier, EXPERTS - 1 + GROUPS - 1)

    def all_of(ref, send, recv):
        return remote(ref, ref, send, recv, dp, me)

    full = {"g": gate_w, "u": up_w, "d": down_w}

    def region(array, z, away, first, count):
        if array == "d":
            group = z * Y + (away + 1) % Y
            return down_w.at[pl.ds(group * piece + first * half, count * half), :]
        group = (zl if z == 0 else 1 - zl) * Y + (y + away + Y) % Y
        return full[array].at[pl.ds(pl.multiple_of(group * piece + first * half, 16), count * half), :]

    order = {RIGHT: ring_messages(RIGHT), LEFT: ring_messages(LEFT)}
    index = {s: {m[:4]: n for n, m in enumerate(order[s])} for s in order}
    side = {RIGHT: 0, LEFT: 1}
    arrived, zx_done = set(), set()

    def start_zx(array):
        n = "gud".index(array)
        c = remote(
            region(array, 0, 0, 0, 2),
            region(array, int(array == "d"), 0, 0, 2),
            zx_send.at[0],
            zx_recv.at[n],
            partner,
            me,
        )
        c.start()

    def wait_zx(array):
        if array not in zx_done:
            zx_done.add(array)
            n = "gud".index(array)
            there = region(array, 1, 0, 0, 2)
            remote(there, there, zx_send.at[0], zx_recv.at[n], partner, me).wait_recv()

    def wait_ring(s, n):
        if (s, n) in arrived:
            return
        arrived.add((s, n))
        array, z, hops, first, count = order[s][n]
        there = region(array, z, -s * (hops + 1), first, count)
        remote(there, there, ring_send.at[side[s], 0], ring_recv.at[side[s], n], dp, me).wait_recv()

    def forward(s, n):
        array, z, hops, first, count = order[s][n]
        if hops:
            if (array, z, hops - 1, first) in index[s]:
                wait_ring(s, index[s][(array, z, hops - 1, first)])
        elif z:
            wait_zx(array)
        src = region(array, z, -s * hops, first, count)
        if array == "d":
            dst = region(array, z, -s * (hops + 1), first, count)
        else:
            dst = region(array, z, -s * hops, first, count)
        c = remote(
            src,
            dst,
            ring_send.at[side[s], int(n >= GATE_UP)],
            ring_recv.at[side[s], n],
            zl * Y + (y + s + Y) % Y,
            me,
        )
        c.start()

    def ring_step(n):
        forward(RIGHT, n)
        forward(LEFT, n)


    def block_of(ref, at):
        return ref.at[pl.ds(pl.multiple_of(at * ZH * CAP, ZH * CAP), ZH * CAP), :]

    def token_copy(n, step):
        return remote(
            token_part[n],
            block_of(token_all[n], zh),
            token_send.at[n],
            token_recv.at[n, step % ZH],
            dp,
            expert_index(x, (zh + step + ZH) % ZH, core),
        )

    def relay_copy(n):
        step = 1 if n == 0 else -1
        at = block_of(token_all[n], (zh - step + ZH) % ZH)
        return remote(
            at,
            at,
            token_send.at[n],
            token_recv.at[n, 2],
            dp,
            expert_index(x, (zh + step + ZH) % ZH, core),
        )

    def wait_tokens(n, step):
        there = block_of(token_all[n], (zh - step + ZH) % ZH)
        remote(there, there, token_send.at[n], token_recv.at[n, step % ZH], dp, me).wait_recv()

    def row_copy(n):
        def copy(k):
            to = (xc + k) % XC
            return remote(
                block_of(outgoing[n], to),
                block_of(rows[n], xc),
                row_send.at[n],
                row_recv.at[n],
                dp,
                expert_index(to // C, zh, to % C),
            )

        return copy

    def gather_send(n, step):
        token_copy(n, step).start()

    def gather_own(n):
        token_all[n][pl.ds(pl.multiple_of(zh * toks, toks), toks), :] = token_part[n][...]

    def rows_send(n):
        wait_tokens(n, -1 if n == 0 else 1)
        wait_tokens(n, 2)
        step = 256

        def some(m, carry):
            at = pl.ds(pl.multiple_of(m * step, step), step)
            outgoing[n][:, at] = dot_down(
                w_wide[2 * ZH * toks :, :], token_all[n][:, at]
            ).astype(BF16)
            return carry

        lax.fori_loop(0, part // step, some, 0)
        starts(row_copy(n), XC)
        at = pl.ds(pl.multiple_of(xc * ZH * CAP, ZH * CAP), ZH * CAP)
        rows[n][at, :] = outgoing[n][at, :]

    def relay(n):
        wait_tokens(n, 1 if n == 0 else -1)
        relay_copy(n).start()

    def rows_take(n):
        all_of(rows[n].at[: (XC - 1) * ZH * CAP], row_send.at[n], row_recv.at[n]).wait_recv()

    def share(n):
        array, away, s, m = SHARED[n]
        wait_ring(s, m)
        c = remote(
            region(array, 0, away, 0, 2),
            region(array, 0, away, 0, 2),
            share_send.at[0],
            share_recv.at[n],
            partner,
            me,
        )
        c.start()

    def wait_share(n):
        array, away, _, _ = SHARED[n]
        there = region(array, 1, away, 0, 2)
        remote(there, there, share_send.at[0], share_recv.at[n], partner, me).wait_recv()

    def w_copy(k):
        to = (zh + k) % ZH
        return remote(w_send.at[to], w_recv.at[zh], w_ssem.at[0], w_rsem.at[0], dp, expert_index(x, to, core))

    def stat_a_copy(k):
        to = (dp + k) % GROUPS
        return remote(stat_mine.at[0], stat_a.at[dp], sa_send.at[0], sa_recv.at[0], to, me)

    def stat_b_copy(k):
        to = (me + k) % EXPERTS
        return remote(stat_mine.at[1], stat_b.at[me], sb_send.at[0], sb_recv.at[0], dp, to)

    def starts(copy, count):
        def one(k, carry):
            copy(k).start()
            return carry

        lax.fori_loop(1, count, one, 0)

    ring_step(0)
    ring_step(1)

    loads[0].wait()
    loads[1].wait()

    lanes = 128
    expert_row = iota((lanes, toks), 0)
    named = jnp.zeros((lanes, toks), F32)
    score = jnp.zeros((lanes, toks), F32)
    for k in range(topk):
        hit = ids[k : k + 1, :] == expert_row
        named = named + jnp.where(hit, 1.0, 0.0)
        score = score + jnp.where(hit, scores[k : k + 1, :], 0.0)
    earlier = (iota((toks, toks), 0) < iota((toks, toks), 1)).astype(F32).astype(BF16)
    named16 = named.astype(BF16)
    rank16 = dot(named16, earlier).astype(BF16)
    score_high = score.astype(BF16)
    rest = score - score_high.astype(F32)
    score_low = rest.astype(BF16)
    score_last = (rest - score_low.astype(F32)).astype(BF16)

    ones = jnp.ones((8, toks), BF16)
    load = dot_across(ones, named16)
    mass = dot_across(ones, score_high) + dot_across(ones, score_low) + dot_across(ones, score_last)
    row8 = iota((8, lanes), 0)
    stat_mine[0] = jnp.where(row8 == 0, load, jnp.where(row8 == 1, mass, 0.0))

    wide = 128
    slot_wide = (iota((toks, wide), 1) & 15).astype(F32)
    for z in range(ZH):
        pick = (iota((lanes, wide), 0) == expert_of(iota((lanes, wide), 1) >> 4, z)).astype(F32).astype(BF16)
        there = dot_down(rank16, pick) == slot_wide
        w_send[z, 0] = jnp.where(there, dot_down(score_high, pick), 0.0).astype(BF16)
        w_send[z, 1] = jnp.where(there, dot_down(score_low, pick), 0.0).astype(BF16)
        w_send[z, 2] = jnp.where(there, dot_down(named16, pick), 0.0).astype(BF16)

    starts(stat_a_copy, GROUPS)
    for k in range(1, ZH):
        w_copy(k).start()
    loads[5].wait()
    loads[6].wait()
    gather_send(0, 1)
    gather_send(1, -1)
    gather_send(1, 1)
    gather_send(0, -1)
    gather_own(0)
    gather_own(1)
    stat_a[dp] = stat_mine[0]
    w_recv[zh] = w_send[zh]

    ring_step(2)
    ring_step(3)
    relay(0)
    relay(1)
    for array in "gud":
        start_zx(array)

    all_of(w_recv.at[: ZH - 1], w_ssem.at[0], w_rsem.at[0]).wait_recv()
    from_slot, to_slot = iota((wide, slots), 0), iota((wide, slots), 1)
    for z in range(ZH):
        widen = (
            ((to_slot >> 6) == (from_slot >> 4))
            & (((to_slot >> 4) & 3) == z)
            & ((to_slot & 15) == (from_slot & 15))
        )
        widen = widen.astype(F32).astype(BF16)
        for kind in range(3):
            w_wide[pl.ds((kind * ZH + z) * toks, toks), :] = dot(w_recv[z, kind], widen).astype(BF16)

    ring_step(4)
    ring_step(5)
    rows_send(0)
    rows_send(1)
    ring_step(6)
    share(0)
    share(1)
    ring_step(7)
    ring_step(8)
    share(2)
    share(3)

    all_of(stat_a.at[: GROUPS - 1], sa_send.at[0], sa_recv.at[0]).wait_recv()
    stat_mine[1] = jnp.sum(stat_a[...], axis=0)
    starts(stat_b_copy, EXPERTS)
    stat_b[me] = stat_mine[1]

    for n in range(9, GATE_UP + 4):
        ring_step(n)

    rows_take(0)
    rows_take(1)
    for n in range(len(SHARED)):
        wait_share(n)
    for s in (RIGHT, LEFT):
        for n in range(GATE_UP):
            wait_ring(s, n)

    part_width = 256
    block = slots // 2
    for n in range(hid // part_width):
        columns = slice(n * part_width, (n + 1) * part_width)

        def hidden_rows(m, carry, columns=columns):
            at = pl.ds(pl.multiple_of(m * block, block), block)
            gate = sum(
                dot(rows[k][at, :], gate_w[k * part : (k + 1) * part, columns]) for k in range(PARTS)
            )
            up = sum(
                dot(rows[k][at, :], up_w[k * part : (k + 1) * part, columns]) for k in range(PARTS)
            )
            hidden[at, columns] = (gate / (1.0 + jnp.exp(-gate)) * up).astype(BF16)
            return carry

        lax.fori_loop(0, slots // block, hidden_rows, 0)
        ring_step(GATE_UP + 4 + n)

    def x_copy(n):
        def copy(k):
            to = (xc + k) % XC
            return remote(
                block_of(produced[n], to),
                block_of(x_in[n], xc),
                xp_send.at[n],
                xp_recv.at[n],
                dp,
                expert_index(to // C, zh, to % C),
            )

        return copy

    def z_copy(n):
        def copy(k):
            to = (zh + k) % ZH
            return remote(
                partial[n].at[to],
                z_in[n].at[zh],
                zp_send.at[n],
                zp_recv.at[n],
                dp,
                expert_index(x, to, core),
            )

        return copy

    def wait_down(z, first, columns):
        needed = range(first // piece, -(-(first + columns) // piece))
        for s in (RIGHT, LEFT):
            for m in range(GATE_UP, MESSAGES):
                if order[s][m][1] == z and (1 - s * (order[s][m][2] + 1)) % Y in needed:
                    wait_ring(s, m)

    def produce(n):
        z, first, columns = CHUNKS[n]
        wait_down(z, first, columns)
        produced[n][...] = dot_across(
            hidden[...], down_w[pl.ds(z * Y * piece + first, columns), :]
        ).astype(BF16)
        starts(x_copy(n), XC)
        at = pl.ds(pl.multiple_of(xc * ZH * CAP, ZH * CAP), ZH * CAP)
        x_in[n][at, :] = produced[n][at, :]

    def combine(n):
        all_of(x_in[n].at[: (XC - 1) * ZH * CAP], xp_send.at[n], xp_recv.at[n]).wait_recv()
        both = dot(w_wide[: 2 * ZH * toks, :], x_in[n][...])
        summed = (both[: ZH * toks] + both[ZH * toks :]).astype(BF16)
        for z in range(ZH):
            partial[n][z] = summed[z * toks : (z + 1) * toks]
        starts(z_copy(n), ZH)
        z_in[n][zh] = partial[n][zh]

    def finish(n):
        all_of(z_in[n].at[: ZH - 1], zp_send.at[n], zp_recv.at[n]).wait_recv()
        result = z_in[n][0].astype(F32)
        for z in range(1, ZH):
            result = result + z_in[n][z].astype(F32)
        z, first, columns = CHUNKS[n]
        relative[z, :, first : first + columns] = result

    def place_columns(z):
        there = pl.multiple_of((zl if z == 0 else 1 - zl) * Y * piece, Y * piece)
        turned = pltpu.roll(relative[z], ((y + Y - 1) % Y) * piece, 1)
        out[:, pl.ds(there, Y * piece)] = turned.astype(BF16)

    produce(0)
    produce(1)
    ring_step(GATE_UP + 7)
    ring_step(GATE_UP + 8)
    combine(0)
    ring_step(GATE_UP + 9)
    produce(2)
    combine(1)
    ring_step(GATE_UP + 10)
    ring_step(GATE_UP + 11)
    combine(2)
    produce(5)
    ring_step(GATE_UP + 12)
    finish(0)
    produce(3)
    produce(4)
    finish(1)
    ring_step(GATE_UP + 13)
    combine(5)
    combine(3)
    all_of(stat_b.at[: EXPERTS - 1], sb_send.at[0], sb_recv.at[0]).wait_recv()
    totals = jnp.sum(stat_b[...], axis=0)
    count, masses = totals[0:1, :], totals[1:2, :]
    total = toks * GROUPS * EXPERTS
    loss = jnp.sum(
        (EXPERTS * count / (topk * total)) * (masses / total), axis=1, keepdims=True
    )
    my_load = jnp.sum(jnp.where(iota((1, lanes), 1) == me, count, 0.0), axis=1, keepdims=True)
    load_out[...] = my_load.astype(I32)
    loss_out[...] = loss

    finish(2)
    produce(6)
    combine(4)
    produce(7)
    produce(8)
    finish(5)
    finish(3)
    combine(6)
    combine(7)
    combine(8)
    finish(4)
    place_columns(0)
    finish(6)
    finish(7)
    finish(8)
    place_columns(1)

    for s in (0, 1):
        all_of(gate_w.at[: GATE_UP * piece], ring_send.at[s, 0], ring_recv.at[s, 0]).wait_send()
        all_of(
            down_w.at[: (MESSAGES - GATE_UP) * half], ring_send.at[s, 1], ring_recv.at[s, 0]
        ).wait_send()
    all_of(gate_w.at[: 3 * piece], zx_send.at[0], zx_recv.at[0]).wait_send()
    all_of(gate_w.at[: len(SHARED) * piece], share_send.at[0], share_recv.at[0]).wait_send()
    all_of(w_recv.at[: ZH - 1], w_ssem.at[0], w_rsem.at[0]).wait_send()
    all_of(stat_a.at[: GROUPS - 1], sa_send.at[0], sa_recv.at[0]).wait_send()
    all_of(stat_b.at[: EXPERTS - 1], sb_send.at[0], sb_recv.at[0]).wait_send()
    for n in range(PARTS):
        all_of(token_all[n].at[: (ZH - 1) * toks], token_send.at[n], token_recv.at[n, 0]).wait_send()
        all_of(rows[n].at[: (XC - 1) * ZH * CAP], row_send.at[n], row_recv.at[n]).wait_send()
    for n in range(len(CHUNKS)):
        all_of(x_in[n].at[: (XC - 1) * ZH * CAP], xp_send.at[n], xp_recv.at[n]).wait_send()
        all_of(z_in[n].at[: ZH - 1], zp_send.at[n], zp_recv.at[n]).wait_send()


def on_device(tokens, expert_ids, gate_scores, w_gate, w_up, w_down):
    toks, width = tokens.shape
    hid = w_gate.shape[2]
    slots = EXPERTS * CAP
    dma = pltpu.SemaphoreType.DMA
    vmem = pl.BlockSpec(memory_space=pltpu.VMEM)
    mixed, load, loss = pl.pallas_call(
        kernel,
        out_shape=(
            jax.ShapeDtypeStruct((toks, width), BF16),
            jax.ShapeDtypeStruct((1, 1), I32),
            jax.ShapeDtypeStruct((1, 1), F32),
        ),
        in_specs=[pl.BlockSpec(memory_space=pl.ANY)] * 6,
        out_specs=(vmem, vmem, vmem),
        scratch_shapes=[
            pltpu.VMEM(expert_ids.shape[::-1], I32),
            pltpu.VMEM(expert_ids.shape[::-1], F32),
            pltpu.VMEM((width, hid), BF16),
            pltpu.VMEM((width, hid), BF16),
            pltpu.VMEM((width, hid), BF16),
            pltpu.VMEM((slots, hid), BF16),
            pltpu.VMEM((ZL, toks, width // ZL), F32),
            pltpu.VMEM((ZH, 3, toks, 128), BF16),
            pltpu.VMEM((ZH, 3, toks, 128), BF16),
            pltpu.VMEM((3 * ZH * toks, slots), BF16),
            pltpu.VMEM((GROUPS, 8, 128), F32),
            pltpu.VMEM((EXPERTS, 8, 128), F32),
            pltpu.VMEM((2, 8, 128), F32),
            dma((7,)),
            dma((2, 2)),
            dma((2, MESSAGES)),
            dma((1,)),
            dma((3,)),
            dma((1,)),
            dma((len(SHARED),)),
            dma((PARTS,)),
            dma((PARTS, ZH)),
            dma((PARTS,)),
            dma((PARTS,)),
            dma((1,)),
            dma((1,)),
            dma((1,)),
            dma((1,)),
            dma((1,)),
            dma((1,)),
            dma((len(CHUNKS),)),
            dma((len(CHUNKS),)),
            dma((len(CHUNKS),)),
            dma((len(CHUNKS),)),
        ]
        + [pltpu.VMEM((toks, width // PARTS), BF16)] * PARTS
        + [pltpu.VMEM((ZH * toks, width // PARTS), BF16)] * PARTS
        + [pltpu.VMEM((slots, width // PARTS), BF16)] * (2 * PARTS)
        + [pltpu.VMEM((slots, w), BF16) for _, _, w in CHUNKS] * 2
        + [pltpu.VMEM((ZH, toks, w), BF16) for _, _, w in CHUNKS] * 2,
        compiler_params=pltpu.CompilerParams(
            collective_id=0, has_side_effects=True, vmem_limit_bytes=60 * 1024 * 1024
        ),
        name="routed_layer",
    )(tokens, expert_ids.T, gate_scores.T, w_gate[0], w_up[0], w_down[0].T)
    return mixed, load[0], loss[0, 0]


def solution(mesh):
    both = ("dp", "expert")
    return jax.shard_map(
        on_device,
        mesh=mesh,
        in_specs=(
            P(both, None),
            P(both, None),
            P(both, None),
            P("expert", "dp", None),
            P("expert", "dp", None),
            P("expert", None, "dp"),
        ),
        out_specs=(P(both, None), P("expert"), P()),
        check_vma=False,
    )
```

```python
import functools

import jax
import jax.numpy as jnp
from jax import lax
from jax.experimental import pallas as pl
from jax.experimental.pallas import tpu as pltpu
from jax.sharding import PartitionSpec as P

F32, BF16, I32 = jnp.float32, jnp.bfloat16, jnp.int32
X, ZH, C, ZL, Y = 4, 4, 2, 2, 8
CAP = 16
XC = X * C
EXPERTS = X * ZH * C
GROUPS = ZL * Y
RIGHT, LEFT = 1, -1
CHUNKS = (
    (0, 0, 128),
    (0, 128, 256),
    (0, 384, 256),
    (0, 1024, 256),
    (1, 0, 384),
    (0, 640, 384),
    (1, 384, 256),
    (1, 1024, 256),
    (1, 640, 256),
    (1, 896, 128),
)


def iota(shape, dim):
    return lax.broadcasted_iota(I32, shape, dim)


def dot(a, b):
    return jnp.dot(a, b, preferred_element_type=F32)


def dot_down(a, b):
    return lax.dot_general(a, b, (((0,), (0,)), ((), ())), preferred_element_type=F32)


def dot_across(a, b):
    return lax.dot_general(a, b, (((1,), (1,)), ((), ())), preferred_element_type=F32)


def remote(src, dst, send, recv, dp, ex):
    return pltpu.make_async_remote_copy(
        src_ref=src,
        dst_ref=dst,
        send_sem=send,
        recv_sem=recv,
        device_id=(dp, ex),
        device_id_type=pl.DeviceIdType.MESH,
    )


def expert_of(xc, zh):
    return ((xc >> 1) * ZH + zh) * C + (xc & 1)


def expert_index(x, zh, core):
    return (x * ZH + zh) * C + core


def ring_messages(direction):
    far = "g" if direction == RIGHT else "u"
    half = 0 if direction == RIGHT else 1
    out = []
    near = "u" if direction == RIGHT else "g"
    for hops in range(3):
        out += [(far, 0, hops, 0, 2), (near, 0, hops, 0, 2)]
    out.append((far, 0, 3, 0, 2))
    for hops in range(2):
        out += [(near, 1, hops, 0, 2), (far, 1, hops, 0, 2)]
    out.append((near, 1, 2, 0, 2))
    for z, hops, first in (
        [(0, 0, half), (0, 0, 1 - half), (0, 1, half), (0, 1, 1 - half)]
        + [(0, 2, half), (0, 2, 1 - half), (0, 3, half)]
        + [(1, 1, half), (1, 1, 1 - half), (1, 2, half), (1, 2, 1 - half), (1, 3, half)]
    ):
        out.append(("d", z, hops, first, 1))
    return out


MESSAGES = len(ring_messages(RIGHT))
GATE_UP = 12
SHARED = (("g", -3, RIGHT, 4), ("u", 3, LEFT, 4), ("g", -4, RIGHT, 6), ("u", 4, LEFT, 6))
SHARED_DOWN = ((-1, 0), (1, 1), (-1, 1), (1, 0))
PARTS = 2


def kernel(
    tokens,
    ids_in,
    scores_in,
    wg,
    wu,
    wd,
    out,
    load_out,
    loss_out,
    ids,
    scores,
    gate_w,
    up_w,
    down_w,
    hidden,
    relative,
    w_send,
    w_recv,
    w_wide,
    stat_a,
    stat_b,
    stat_mine,
    load_sem,
    ring_send,
    ring_recv,
    zx_send,
    zx_recv,
    share_send,
    share_recv,
    token_send,
    token_recv,
    row_send,
    row_recv,
    w_ssem,
    w_rsem,
    sa_send,
    sa_recv,
    sb_send,
    sb_recv,
    xp_send,
    xp_recv,
    zp_send,
    zp_recv,
    *buffers,
):
    (token_part, token_all, outgoing, rows), chunk_buffers = (
        [buffers[n * PARTS : (n + 1) * PARTS] for n in range(4)],
        buffers[4 * PARTS :],
    )
    produced, x_in, partial, z_in = (
        chunk_buffers[n * len(CHUNKS) : (n + 1) * len(CHUNKS)] for n in range(4)
    )
    toks, width = tokens.shape
    piece, hid = wg.shape
    half = piece // 2
    slots = EXPERTS * CAP
    topk = ids.shape[0]

    dp = lax.axis_index("dp")
    me = lax.axis_index("expert")
    zl, y = dp // Y, dp % Y
    core, zh, x = me % C, (me // C) % ZH, me // (C * ZH)
    xc = x * C + core
    partner = (1 - zl) * Y + y

    part = width // PARTS
    mine = pl.ds(pl.multiple_of(dp * piece, 16), piece)
    loads = [
        pltpu.make_async_copy(source, target, load_sem.at[n])
        for n, (source, target) in enumerate(
            [(ids_in, ids), (scores_in, scores)]
            + [(wg, gate_w.at[mine, :]), (wu, up_w.at[mine, :]), (wd, down_w.at[pl.ds(piece, piece), :])]
            + [(tokens.at[:, n * part : (n + 1) * part], token_part[n]) for n in range(PARTS)]
        )
    ]
    for c in loads:
        c.start()

    barrier = pltpu.get_barrier_semaphore()

    def greet_expert(k, carry):
        pl.semaphore_signal(
            barrier, inc=1, device_id=(dp, (me + k) % EXPERTS), device_id_type=pl.DeviceIdType.MESH
        )
        return carry

    def greet_group(k, carry):
        pl.semaphore_signal(
            barrier, inc=1, device_id=((dp + k) % GROUPS, me), device_id_type=pl.DeviceIdType.MESH
        )
        return carry

    lax.fori_loop(1, GROUPS, greet_group, 0)
    lax.fori_loop(1, EXPERTS, greet_expert, 0)

    for c in loads[2:5]:
        c.wait()

    pl.semaphore_wait(barrier, EXPERTS - 1 + GROUPS - 1)

    def all_of(ref, send, recv):
        return remote(ref, ref, send, recv, dp, me)

    full = {"g": gate_w, "u": up_w, "d": down_w}

    def region(array, z, away, first, count):
        if array == "d":
            group = z * Y + (away + 1) % Y
            return down_w.at[pl.ds(group * piece + first * half, count * half), :]
        group = (zl if z == 0 else 1 - zl) * Y + (y + away + Y) % Y
        return full[array].at[pl.ds(pl.multiple_of(group * piece + first * half, 16), count * half), :]

    order = {RIGHT: ring_messages(RIGHT), LEFT: ring_messages(LEFT)}
    index = {s: {m[:4]: n for n, m in enumerate(order[s])} for s in order}
    side = {RIGHT: 0, LEFT: 1}
    arrived, zx_done, shared_down = set(), set(), set()

    def start_zx(array):
        n = "gud".index(array)
        c = remote(
            region(array, 0, 0, 0, 2),
            region(array, int(array == "d"), 0, 0, 2),
            zx_send.at[0],
            zx_recv.at[n],
            partner,
            me,
        )
        c.start()

    def wait_zx(array):
        if array not in zx_done:
            zx_done.add(array)
            n = "gud".index(array)
            there = region(array, 1, 0, 0, 2)
            remote(there, there, zx_send.at[0], zx_recv.at[n], partner, me).wait_recv()

    def wait_ring(s, n):
        if (s, n) in arrived:
            return
        arrived.add((s, n))
        array, z, hops, first, count = order[s][n]
        there = region(array, z, -s * (hops + 1), first, count)
        remote(there, there, ring_send.at[side[s], 0], ring_recv.at[side[s], n], dp, me).wait_recv()

    def share_down(n):
        away, first = SHARED_DOWN[n]
        wait_ring(-away, index[-away][("d", 0, 0, first)])
        remote(
            region("d", 0, away, first, 1),
            region("d", 1, away, first, 1),
            share_send.at[1],
            share_recv.at[len(SHARED) + n],
            partner,
            me,
        ).start()

    def wait_share_down(away, first):
        n = SHARED_DOWN.index((away, first))
        if n not in shared_down:
            shared_down.add(n)
            there = region("d", 1, away, first, 1)
            remote(there, there, share_send.at[1], share_recv.at[len(SHARED) + n], partner, me).wait_recv()

    def forward(s, n):
        array, z, hops, first, count = order[s][n]
        if array == "d" and z == 1 and hops == 1:
            wait_share_down(-s, first)
        elif hops:
            if (array, z, hops - 1, first) in index[s]:
                wait_ring(s, index[s][(array, z, hops - 1, first)])
        elif z:
            wait_zx(array)
        src = region(array, z, -s * hops, first, count)
        if array == "d":
            dst = region(array, z, -s * (hops + 1), first, count)
        else:
            dst = region(array, z, -s * hops, first, count)
        c = remote(
            src,
            dst,
            ring_send.at[side[s], int(n >= GATE_UP)],
            ring_recv.at[side[s], n],
            zl * Y + (y + s + Y) % Y,
            me,
        )
        c.start()

    def ring_step(n):
        forward(RIGHT, n)
        forward(LEFT, n)


    def block_of(ref, at):
        return ref.at[pl.ds(pl.multiple_of(at * ZH * CAP, ZH * CAP), ZH * CAP), :]

    def token_copy(n, step):
        return remote(
            token_part[n],
            block_of(token_all[n], zh),
            token_send.at[n],
            token_recv.at[n, step % ZH],
            dp,
            expert_index(x, (zh + step + ZH) % ZH, core),
        )

    def relay_copy(n):
        step = 1 if n == 0 else -1
        at = block_of(token_all[n], (zh - step + ZH) % ZH)
        return remote(
            at,
            at,
            token_send.at[n],
            token_recv.at[n, 2],
            dp,
            expert_index(x, (zh + step + ZH) % ZH, core),
        )

    def wait_tokens(n, step):
        there = block_of(token_all[n], (zh - step + ZH) % ZH)
        remote(there, there, token_send.at[n], token_recv.at[n, step % ZH], dp, me).wait_recv()

    def row_copy(n):
        def copy(k):
            to = (xc + k) % XC
            return remote(
                block_of(outgoing[n], to),
                block_of(rows[n], xc),
                row_send.at[n],
                row_recv.at[n],
                dp,
                expert_index(to // C, zh, to % C),
            )

        return copy

    def gather_send(n, step):
        token_copy(n, step).start()

    def gather_own(n):
        token_all[n][pl.ds(pl.multiple_of(zh * toks, toks), toks), :] = token_part[n][...]

    def rows_send(n):
        wait_tokens(n, -1 if n == 0 else 1)
        wait_tokens(n, 2)
        step = 256

        def some(m, carry):
            at = pl.ds(pl.multiple_of(m * step, step), step)
            outgoing[n][:, at] = dot_down(
                w_wide[2 * ZH * toks :, :], token_all[n][:, at]
            ).astype(BF16)
            return carry

        lax.fori_loop(0, part // step, some, 0)
        starts(row_copy(n), XC)
        at = pl.ds(pl.multiple_of(xc * ZH * CAP, ZH * CAP), ZH * CAP)
        rows[n][at, :] = outgoing[n][at, :]

    def relay(n):
        wait_tokens(n, 1 if n == 0 else -1)
        relay_copy(n).start()

    def rows_take(n):
        all_of(rows[n].at[: (XC - 1) * ZH * CAP], row_send.at[n], row_recv.at[n]).wait_recv()

    def share(n):
        array, away, s, m = SHARED[n]
        wait_ring(s, m)
        c = remote(
            region(array, 0, away, 0, 2),
            region(array, 0, away, 0, 2),
            share_send.at[0],
            share_recv.at[n],
            partner,
            me,
        )
        c.start()

    def wait_share(n):
        array, away, _, _ = SHARED[n]
        there = region(array, 1, away, 0, 2)
        remote(there, there, share_send.at[0], share_recv.at[n], partner, me).wait_recv()

    def w_copy(k):
        to = (zh + k) % ZH
        return remote(w_send.at[to], w_recv.at[zh], w_ssem.at[0], w_rsem.at[0], dp, expert_index(x, to, core))

    def stat_a_copy(k):
        to = (dp + k) % GROUPS
        return remote(stat_mine.at[0], stat_a.at[dp], sa_send.at[0], sa_recv.at[0], to, me)

    def stat_b_copy(k):
        to = (me + k) % EXPERTS
        return remote(stat_mine.at[1], stat_b.at[me], sb_send.at[0], sb_recv.at[0], dp, to)

    def starts(copy, count):
        def one(k, carry):
            copy(k).start()
            return carry

        lax.fori_loop(1, count, one, 0)

    ring_step(0)
    ring_step(1)

    loads[5].wait()
    loads[6].wait()
    gather_send(0, 1)
    gather_send(1, -1)
    gather_send(1, 1)
    gather_send(0, -1)
    gather_own(0)
    gather_own(1)

    loads[0].wait()
    loads[1].wait()

    lanes = 128
    expert_row = iota((lanes, toks), 0)
    named = jnp.zeros((lanes, toks), F32)
    score = jnp.zeros((lanes, toks), F32)
    for k in range(topk):
        hit = ids[k : k + 1, :] == expert_row
        named = named + jnp.where(hit, 1.0, 0.0)
        score = score + jnp.where(hit, scores[k : k + 1, :], 0.0)
    earlier = (iota((toks, toks), 0) < iota((toks, toks), 1)).astype(F32).astype(BF16)
    named16 = named.astype(BF16)
    rank16 = dot(named16, earlier).astype(BF16)
    score_high = score.astype(BF16)
    rest = score - score_high.astype(F32)
    score_low = rest.astype(BF16)
    score_last = (rest - score_low.astype(F32)).astype(BF16)

    ones = jnp.ones((8, toks), BF16)
    load = dot_across(ones, named16)
    mass = dot_across(ones, score_high) + dot_across(ones, score_low) + dot_across(ones, score_last)
    row8 = iota((8, lanes), 0)
    stat_mine[0] = jnp.where(row8 == 0, load, jnp.where(row8 == 1, mass, 0.0))

    wide = 128
    slot_wide = (iota((toks, wide), 1) & 15).astype(F32)
    for z in range(ZH):
        pick = (iota((lanes, wide), 0) == expert_of(iota((lanes, wide), 1) >> 4, z)).astype(F32).astype(BF16)
        there = dot_down(rank16, pick) == slot_wide
        w_send[z, 0] = jnp.where(there, dot_down(score_high, pick), 0.0).astype(BF16)
        w_send[z, 1] = jnp.where(there, dot_down(score_low, pick), 0.0).astype(BF16)
        w_send[z, 2] = jnp.where(there, dot_down(named16, pick), 0.0).astype(BF16)

    starts(stat_a_copy, GROUPS)
    for k in range(1, ZH):
        w_copy(k).start()
    stat_a[dp] = stat_mine[0]
    w_recv[zh] = w_send[zh]

    ring_step(2)
    ring_step(3)
    relay(0)
    relay(1)
    for array in "gud":
        start_zx(array)

    ring_step(4)
    ring_step(5)

    all_of(w_recv.at[: ZH - 1], w_ssem.at[0], w_rsem.at[0]).wait_recv()
    from_slot, to_slot = iota((wide, slots), 0), iota((wide, slots), 1)
    for z in range(ZH):
        widen = (
            ((to_slot >> 6) == (from_slot >> 4))
            & (((to_slot >> 4) & 3) == z)
            & ((to_slot & 15) == (from_slot & 15))
        )
        widen = widen.astype(F32).astype(BF16)
        for kind in range(3):
            w_wide[pl.ds((kind * ZH + z) * toks, toks), :] = dot(w_recv[z, kind], widen).astype(BF16)

    rows_send(0)
    rows_send(1)
    ring_step(6)
    share(0)
    share(1)
    ring_step(7)
    ring_step(8)
    share(2)
    share(3)

    all_of(stat_a.at[: GROUPS - 1], sa_send.at[0], sa_recv.at[0]).wait_recv()
    stat_mine[1] = jnp.sum(stat_a[...], axis=0)
    starts(stat_b_copy, EXPERTS)
    stat_b[me] = stat_mine[1]

    for n in range(9, GATE_UP + 2):
        ring_step(n)

    rows_take(0)
    rows_take(1)
    for n in range(len(SHARED)):
        wait_share(n)
    for s in (RIGHT, LEFT):
        for n in range(GATE_UP):
            wait_ring(s, n)

    part_width = 256
    block = slots // 2
    def hidden_part(n, m):
        columns, at = slice(n * part_width, (n + 1) * part_width), slice(m * block, (m + 1) * block)
        gate = sum(
            dot(rows[k][at, :], gate_w[k * part : (k + 1) * part, columns]) for k in range(PARTS)
        )
        up = sum(dot(rows[k][at, :], up_w[k * part : (k + 1) * part, columns]) for k in range(PARTS))
        hidden[at, columns] = (gate / (1.0 + jnp.exp(-gate)) * up).astype(BF16)

    pieces = [(n, m) for n in range(hid // part_width) for m in range(slots // block)]
    for turn in range(2):
        for n, m in pieces[turn * len(pieces) // 2 : (turn + 1) * len(pieces) // 2]:
            hidden_part(n, m)
        ring_step(GATE_UP + 2 + turn)
        share_down(2 * turn)
        share_down(2 * turn + 1)

    def x_copy(n):
        def copy(k):
            to = (xc + k) % XC
            return remote(
                block_of(produced[n], to),
                block_of(x_in[n], xc),
                xp_send.at[n],
                xp_recv.at[n],
                dp,
                expert_index(to // C, zh, to % C),
            )

        return copy

    def z_copy(n):
        def copy(k):
            to = (zh + k) % ZH
            return remote(
                partial[n].at[to],
                z_in[n].at[zh],
                zp_send.at[n],
                zp_recv.at[n],
                dp,
                expert_index(x, to, core),
            )

        return copy

    def wait_down(z, first, columns):
        needed = range(first // piece, -(-(first + columns) // piece))
        if z == 1 and 1 in needed:
            wait_zx("d")
        for away, part_of in SHARED_DOWN:
            if z == 1 and (away + 1) % Y in needed:
                wait_share_down(away, part_of)
        for s in (RIGHT, LEFT):
            for m in range(GATE_UP, MESSAGES):
                if order[s][m][1] == z and (1 - s * (order[s][m][2] + 1)) % Y in needed:
                    wait_ring(s, m)

    def produce(n):
        z, first, columns = CHUNKS[n]
        wait_down(z, first, columns)
        produced[n][...] = dot_across(
            hidden[...], down_w[pl.ds(z * Y * piece + first, columns), :]
        ).astype(BF16)
        starts(x_copy(n), XC)
        at = pl.ds(pl.multiple_of(xc * ZH * CAP, ZH * CAP), ZH * CAP)
        x_in[n][at, :] = produced[n][at, :]

    def combine(n):
        all_of(x_in[n].at[: (XC - 1) * ZH * CAP], xp_send.at[n], xp_recv.at[n]).wait_recv()
        both = dot(w_wide[: 2 * ZH * toks, :], x_in[n][...])
        summed = (both[: ZH * toks] + both[ZH * toks :]).astype(BF16)
        for z in range(ZH):
            partial[n][z] = summed[z * toks : (z + 1) * toks]
        starts(z_copy(n), ZH)
        z_in[n][zh] = partial[n][zh]

    def finish(n):
        all_of(z_in[n].at[: ZH - 1], zp_send.at[n], zp_recv.at[n]).wait_recv()
        result = z_in[n][0].astype(F32)
        for z in range(1, ZH):
            result = result + z_in[n][z].astype(F32)
        z, first, columns = CHUNKS[n]
        relative[z, :, first : first + columns] = result

    def place_columns(z):
        there = pl.multiple_of((zl if z == 0 else 1 - zl) * Y * piece, Y * piece)
        turned = pltpu.roll(relative[z], ((y + Y - 1) % Y) * piece, 1)
        out[:, pl.ds(there, Y * piece)] = turned.astype(BF16)

    produce(0)
    produce(1)
    ring_step(GATE_UP + 4)
    combine(0)
    ring_step(GATE_UP + 5)
    produce(2)
    ring_step(GATE_UP + 6)
    combine(1)
    ring_step(GATE_UP + 7)
    ring_step(GATE_UP + 8)
    produce(3)
    produce(4)
    combine(2)
    produce(5)
    ring_step(GATE_UP + 9)
    combine(3)
    ring_step(GATE_UP + 10)
    produce(6)
    finish(0)
    finish(1)
    ring_step(GATE_UP + 11)
    combine(4)
    finish(2)
    produce(7)
    combine(5)
    produce(8)
    produce(9)
    all_of(stat_b.at[: EXPERTS - 1], sb_send.at[0], sb_recv.at[0]).wait_recv()
    totals = jnp.sum(stat_b[...], axis=0)
    count, masses = totals[0:1, :], totals[1:2, :]
    total = toks * GROUPS * EXPERTS
    loss = jnp.sum(
        (EXPERTS * count / (topk * total)) * (masses / total), axis=1, keepdims=True
    )
    my_load = jnp.sum(jnp.where(iota((1, lanes), 1) == me, count, 0.0), axis=1, keepdims=True)
    load_out[...] = my_load.astype(I32)
    loss_out[...] = loss

    combine(6)
    combine(7)
    combine(8)
    combine(9)
    finish(3)
    finish(4)
    finish(5)
    place_columns(0)
    for n in range(6, len(CHUNKS)):
        finish(n)
    place_columns(1)

    for s in (0, 1):
        all_of(gate_w.at[: GATE_UP * piece], ring_send.at[s, 0], ring_recv.at[s, 0]).wait_send()
        all_of(
            down_w.at[: (MESSAGES - GATE_UP) * half], ring_send.at[s, 1], ring_recv.at[s, 0]
        ).wait_send()
    all_of(gate_w.at[: 3 * piece], zx_send.at[0], zx_recv.at[0]).wait_send()
    all_of(gate_w.at[: len(SHARED) * piece], share_send.at[0], share_recv.at[0]).wait_send()
    all_of(down_w.at[: len(SHARED_DOWN) * half], share_send.at[1], share_recv.at[0]).wait_send()
    all_of(w_recv.at[: ZH - 1], w_ssem.at[0], w_rsem.at[0]).wait_send()
    all_of(stat_a.at[: GROUPS - 1], sa_send.at[0], sa_recv.at[0]).wait_send()
    all_of(stat_b.at[: EXPERTS - 1], sb_send.at[0], sb_recv.at[0]).wait_send()
    for n in range(PARTS):
        all_of(token_all[n].at[: (ZH - 1) * toks], token_send.at[n], token_recv.at[n, 0]).wait_send()
        all_of(rows[n].at[: (XC - 1) * ZH * CAP], row_send.at[n], row_recv.at[n]).wait_send()
    for n in range(len(CHUNKS)):
        all_of(x_in[n].at[: (XC - 1) * ZH * CAP], xp_send.at[n], xp_recv.at[n]).wait_send()
        all_of(z_in[n].at[: ZH - 1], zp_send.at[n], zp_recv.at[n]).wait_send()


def on_device(tokens, expert_ids, gate_scores, w_gate, w_up, w_down):
    toks, width = tokens.shape
    hid = w_gate.shape[2]
    slots = EXPERTS * CAP
    dma = pltpu.SemaphoreType.DMA
    vmem = pl.BlockSpec(memory_space=pltpu.VMEM)
    mixed, load, loss = pl.pallas_call(
        kernel,
        out_shape=(
            jax.ShapeDtypeStruct((toks, width), BF16),
            jax.ShapeDtypeStruct((1, 1), I32),
            jax.ShapeDtypeStruct((1, 1), F32),
        ),
        in_specs=[pl.BlockSpec(memory_space=pl.ANY)] * 6,
        out_specs=(vmem, vmem, vmem),
        scratch_shapes=[
            pltpu.VMEM(expert_ids.shape[::-1], I32),
            pltpu.VMEM(expert_ids.shape[::-1], F32),
            pltpu.VMEM((width, hid), BF16),
            pltpu.VMEM((width, hid), BF16),
            pltpu.VMEM((width, hid), BF16),
            pltpu.VMEM((slots, hid), BF16),
            pltpu.VMEM((ZL, toks, width // ZL), F32),
            pltpu.VMEM((ZH, 3, toks, 128), BF16),
            pltpu.VMEM((ZH, 3, toks, 128), BF16),
            pltpu.VMEM((3 * ZH * toks, slots), BF16),
            pltpu.VMEM((GROUPS, 8, 128), F32),
            pltpu.VMEM((EXPERTS, 8, 128), F32),
            pltpu.VMEM((2, 8, 128), F32),
            dma((7,)),
            dma((2, 2)),
            dma((2, MESSAGES)),
            dma((1,)),
            dma((3,)),
            dma((2,)),
            dma((len(SHARED) + len(SHARED_DOWN),)),
            dma((PARTS,)),
            dma((PARTS, ZH)),
            dma((PARTS,)),
            dma((PARTS,)),
            dma((1,)),
            dma((1,)),
            dma((1,)),
            dma((1,)),
            dma((1,)),
            dma((1,)),
            dma((len(CHUNKS),)),
            dma((len(CHUNKS),)),
            dma((len(CHUNKS),)),
            dma((len(CHUNKS),)),
        ]
        + [pltpu.VMEM((toks, width // PARTS), BF16)] * PARTS
        + [pltpu.VMEM((ZH * toks, width // PARTS), BF16)] * PARTS
        + [pltpu.VMEM((slots, width // PARTS), BF16)] * (2 * PARTS)
        + [pltpu.VMEM((slots, w), BF16) for _, _, w in CHUNKS] * 2
        + [pltpu.VMEM((ZH, toks, w), BF16) for _, _, w in CHUNKS] * 2,
        compiler_params=pltpu.CompilerParams(
            collective_id=0, has_side_effects=True, vmem_limit_bytes=60 * 1024 * 1024
        ),
        name="routed_layer",
    )(tokens, expert_ids.T, gate_scores.T, w_gate[0], w_up[0], w_down[0].T)
    return mixed, load[0], loss[0, 0]


def solution(mesh):
    both = ("dp", "expert")
    return jax.shard_map(
        on_device,
        mesh=mesh,
        in_specs=(
            P(both, None),
            P(both, None),
            P(both, None),
            P("expert", "dp", None),
            P("expert", "dp", None),
            P("expert", None, "dp"),
        ),
        out_specs=(P(both, None), P("expert"), P()),
        check_vma=False,
    )
```

```python
import functools

import jax
import jax.numpy as jnp
from jax import lax
from jax.experimental import pallas as pl
from jax.experimental.pallas import tpu as pltpu
from jax.sharding import PartitionSpec as P

F32, BF16, I32 = jnp.float32, jnp.bfloat16, jnp.int32
X, ZH, C, ZL, Y = 4, 4, 2, 2, 8
CAP = 16
XC = X * C
EXPERTS = X * ZH * C
GROUPS = ZL * Y
RIGHT, LEFT = 1, -1
CHUNKS = (
    (0, 0, 128),
    (0, 128, 256),
    (0, 384, 256),
    (0, 1024, 256),
    (1, 0, 384),
    (0, 640, 384),
    (1, 384, 256),
    (1, 1024, 256),
    (1, 640, 256),
    (1, 896, 128),
)


def iota(shape, dim):
    return lax.broadcasted_iota(I32, shape, dim)


def dot(a, b):
    return jnp.dot(a, b, preferred_element_type=F32)


def dot_down(a, b):
    return lax.dot_general(a, b, (((0,), (0,)), ((), ())), preferred_element_type=F32)


def dot_across(a, b):
    return lax.dot_general(a, b, (((1,), (1,)), ((), ())), preferred_element_type=F32)


def remote(src, dst, send, recv, dp, ex):
    return pltpu.make_async_remote_copy(
        src_ref=src,
        dst_ref=dst,
        send_sem=send,
        recv_sem=recv,
        device_id=(dp, ex),
        device_id_type=pl.DeviceIdType.MESH,
    )


def expert_of(xc, zh):
    return ((xc >> 1) * ZH + zh) * C + (xc & 1)


def expert_index(x, zh, core):
    return (x * ZH + zh) * C + core


def ring_messages(direction):
    far = "g" if direction == RIGHT else "u"
    half = 0 if direction == RIGHT else 1
    out = []
    near = "u" if direction == RIGHT else "g"
    for hops in range(3):
        out += [(far, 0, hops, 0, 2), (near, 0, hops, 0, 2)]
    out.append((far, 0, 3, 0, 2))
    for hops in range(2):
        out += [(near, 1, hops, 0, 2), (far, 1, hops, 0, 2)]
    out.append((near, 1, 2, 0, 2))
    for z, hops, first in (
        [(0, 0, half), (0, 0, 1 - half), (0, 1, half), (0, 1, 1 - half)]
        + [(0, 2, half), (0, 2, 1 - half), (0, 3, half)]
        + [(1, 1, half), (1, 1, 1 - half), (1, 2, half), (1, 2, 1 - half), (1, 3, half)]
    ):
        out.append(("d", z, hops, first, 1))
    return out


MESSAGES = len(ring_messages(RIGHT))
GATE_UP = 12
SHARED = (("g", -3, RIGHT, 4), ("u", 3, LEFT, 4), ("g", -4, RIGHT, 6), ("u", 4, LEFT, 6))
SHARED_DOWN = ((-1, 0), (1, 1), (-1, 1), (1, 0))
PARTS = 2


def kernel(
    tokens,
    ids_in,
    scores_in,
    wg,
    wu,
    wd,
    out,
    load_out,
    loss_out,
    ids,
    scores,
    gate_w,
    up_w,
    down_w,
    hidden,
    relative,
    w_send,
    w_recv,
    w_wide,
    stat_a,
    stat_b,
    stat_mine,
    load_sem,
    ring_send,
    ring_recv,
    zx_send,
    zx_recv,
    share_send,
    share_recv,
    token_send,
    token_recv,
    row_send,
    row_recv,
    w_ssem,
    w_rsem,
    sa_send,
    sa_recv,
    sb_send,
    sb_recv,
    xp_send,
    xp_recv,
    zp_send,
    zp_recv,
    *buffers,
):
    (token_part, token_all, outgoing, rows), chunk_buffers = (
        [buffers[n * PARTS : (n + 1) * PARTS] for n in range(4)],
        buffers[4 * PARTS :],
    )
    produced, x_in, partial, z_in = (
        chunk_buffers[n * len(CHUNKS) : (n + 1) * len(CHUNKS)] for n in range(4)
    )
    toks, width = tokens.shape
    piece, hid = wg.shape
    half = piece // 2
    slots = EXPERTS * CAP
    topk = ids.shape[0]

    dp = lax.axis_index("dp")
    me = lax.axis_index("expert")
    zl, y = dp // Y, dp % Y
    core, zh, x = me % C, (me // C) % ZH, me // (C * ZH)
    xc = x * C + core
    partner = (1 - zl) * Y + y

    part = width // PARTS
    mine = pl.ds(pl.multiple_of(dp * piece, 16), piece)
    loads = [
        pltpu.make_async_copy(source, target, load_sem.at[n])
        for n, (source, target) in enumerate(
            [(ids_in, ids), (scores_in, scores)]
            + [(wg, gate_w.at[mine, :]), (wu, up_w.at[mine, :]), (wd, down_w.at[pl.ds(piece, piece), :])]
            + [(tokens.at[:, n * part : (n + 1) * part], token_part[n]) for n in range(PARTS)]
        )
    ]
    for c in loads:
        c.start()

    barrier = pltpu.get_barrier_semaphore()

    def greet_expert(k, carry):
        pl.semaphore_signal(
            barrier, inc=1, device_id=(dp, (me + k) % EXPERTS), device_id_type=pl.DeviceIdType.MESH
        )
        return carry

    def greet_group(k, carry):
        pl.semaphore_signal(
            barrier, inc=1, device_id=((dp + k) % GROUPS, me), device_id_type=pl.DeviceIdType.MESH
        )
        return carry

    lax.fori_loop(1, GROUPS, greet_group, 0)
    lax.fori_loop(1, EXPERTS, greet_expert, 0)

    for c in loads[2:5]:
        c.wait()

    pl.semaphore_wait(barrier, EXPERTS - 1 + GROUPS - 1)

    def all_of(ref, send, recv):
        return remote(ref, ref, send, recv, dp, me)

    full = {"g": gate_w, "u": up_w, "d": down_w}

    def region(array, z, away, first, count):
        if array == "d":
            group = z * Y + (away + 1) % Y
            return down_w.at[pl.ds(group * piece + first * half, count * half), :]
        group = (zl if z == 0 else 1 - zl) * Y + (y + away + Y) % Y
        return full[array].at[pl.ds(pl.multiple_of(group * piece + first * half, 16), count * half), :]

    order = {RIGHT: ring_messages(RIGHT), LEFT: ring_messages(LEFT)}
    index = {s: {m[:4]: n for n, m in enumerate(order[s])} for s in order}
    side = {RIGHT: 0, LEFT: 1}
    arrived, zx_done, shared_down = set(), set(), set()

    def start_zx(array):
        n = "gud".index(array)
        c = remote(
            region(array, 0, 0, 0, 2),
            region(array, int(array == "d"), 0, 0, 2),
            zx_send.at[0],
            zx_recv.at[n],
            partner,
            me,
        )
        c.start()

    def wait_zx(array):
        if array not in zx_done:
            zx_done.add(array)
            n = "gud".index(array)
            there = region(array, 1, 0, 0, 2)
            remote(there, there, zx_send.at[0], zx_recv.at[n], partner, me).wait_recv()

    def wait_ring(s, n):
        if (s, n) in arrived:
            return
        arrived.add((s, n))
        array, z, hops, first, count = order[s][n]
        there = region(array, z, -s * (hops + 1), first, count)
        remote(there, there, ring_send.at[side[s], 0], ring_recv.at[side[s], n], dp, me).wait_recv()

    def share_down(n):
        away, first = SHARED_DOWN[n]
        wait_ring(-away, index[-away][("d", 0, 0, first)])
        remote(
            region("d", 0, away, first, 1),
            region("d", 1, away, first, 1),
            share_send.at[1],
            share_recv.at[len(SHARED) + n],
            partner,
            me,
        ).start()

    def wait_share_down(away, first):
        n = SHARED_DOWN.index((away, first))
        if n not in shared_down:
            shared_down.add(n)
            there = region("d", 1, away, first, 1)
            remote(there, there, share_send.at[1], share_recv.at[len(SHARED) + n], partner, me).wait_recv()

    def forward(s, n):
        array, z, hops, first, count = order[s][n]
        if array == "d" and z == 1 and hops == 1:
            wait_share_down(-s, first)
        elif hops:
            if (array, z, hops - 1, first) in index[s]:
                wait_ring(s, index[s][(array, z, hops - 1, first)])
        elif z:
            wait_zx(array)
        src = region(array, z, -s * hops, first, count)
        if array == "d":
            dst = region(array, z, -s * (hops + 1), first, count)
        else:
            dst = region(array, z, -s * hops, first, count)
        c = remote(
            src,
            dst,
            ring_send.at[side[s], int(n >= GATE_UP)],
            ring_recv.at[side[s], n],
            zl * Y + (y + s + Y) % Y,
            me,
        )
        c.start()

    def ring_step(n):
        forward(RIGHT, n)
        forward(LEFT, n)


    def block_of(ref, at):
        return ref.at[pl.ds(pl.multiple_of(at * ZH * CAP, ZH * CAP), ZH * CAP), :]

    def token_copy(n, step):
        return remote(
            token_part[n],
            block_of(token_all[n], zh),
            token_send.at[n],
            token_recv.at[n, step % ZH],
            dp,
            expert_index(x, (zh + step + ZH) % ZH, core),
        )

    def relay_copy(n):
        step = 1 if n == 0 else -1
        at = block_of(token_all[n], (zh - step + ZH) % ZH)
        return remote(
            at,
            at,
            token_send.at[n],
            token_recv.at[n, 2],
            dp,
            expert_index(x, (zh + step + ZH) % ZH, core),
        )

    def wait_tokens(n, step):
        there = block_of(token_all[n], (zh - step + ZH) % ZH)
        remote(there, there, token_send.at[n], token_recv.at[n, step % ZH], dp, me).wait_recv()

    def row_copy(n):
        def copy(k):
            to = (xc + k) % XC
            return remote(
                block_of(outgoing[n], to),
                block_of(rows[n], xc),
                row_send.at[n],
                row_recv.at[n],
                dp,
                expert_index(to // C, zh, to % C),
            )

        return copy

    def gather_send(n, step):
        token_copy(n, step).start()

    def gather_own(n):
        token_all[n][pl.ds(pl.multiple_of(zh * toks, toks), toks), :] = token_part[n][...]

    def rows_send(n):
        wait_tokens(n, -1 if n == 0 else 1)
        wait_tokens(n, 2)
        step = 256

        def some(m, carry):
            at = pl.ds(pl.multiple_of(m * step, step), step)
            outgoing[n][:, at] = dot_down(
                w_wide[2 * ZH * toks :, :], token_all[n][:, at]
            ).astype(BF16)
            return carry

        lax.fori_loop(0, part // step, some, 0)
        starts(row_copy(n), XC)
        at = pl.ds(pl.multiple_of(xc * ZH * CAP, ZH * CAP), ZH * CAP)
        rows[n][at, :] = outgoing[n][at, :]

    def relay(n):
        wait_tokens(n, 1 if n == 0 else -1)
        relay_copy(n).start()

    def rows_take(n):
        all_of(rows[n].at[: (XC - 1) * ZH * CAP], row_send.at[n], row_recv.at[n]).wait_recv()

    def share(n):
        array, away, s, m = SHARED[n]
        wait_ring(s, m)
        c = remote(
            region(array, 0, away, 0, 2),
            region(array, 0, away, 0, 2),
            share_send.at[0],
            share_recv.at[n],
            partner,
            me,
        )
        c.start()

    def wait_share(n):
        array, away, _, _ = SHARED[n]
        there = region(array, 1, away, 0, 2)
        remote(there, there, share_send.at[0], share_recv.at[n], partner, me).wait_recv()

    def w_copy(k):
        to = (zh + k) % ZH
        return remote(w_send.at[to], w_recv.at[zh], w_ssem.at[0], w_rsem.at[0], dp, expert_index(x, to, core))

    def stat_a_copy(k):
        to = (dp + k) % GROUPS
        return remote(stat_mine.at[0], stat_a.at[dp], sa_send.at[0], sa_recv.at[0], to, me)

    def stat_b_copy(k):
        to = (me + k) % EXPERTS
        return remote(stat_mine.at[1], stat_b.at[me], sb_send.at[0], sb_recv.at[0], dp, to)

    def starts(copy, count):
        def one(k, carry):
            copy(k).start()
            return carry

        lax.fori_loop(1, count, one, 0)

    ring_step(0)
    ring_step(1)

    loads[5].wait()
    loads[6].wait()
    gather_send(0, 1)
    gather_send(1, -1)
    gather_send(1, 1)
    gather_send(0, -1)
    gather_own(0)
    gather_own(1)

    loads[0].wait()
    loads[1].wait()

    lanes = 128
    expert_row = iota((lanes, toks), 0)
    named = jnp.zeros((lanes, toks), F32)
    score = jnp.zeros((lanes, toks), F32)
    for k in range(topk):
        hit = ids[k : k + 1, :] == expert_row
        named = named + jnp.where(hit, 1.0, 0.0)
        score = score + jnp.where(hit, scores[k : k + 1, :], 0.0)
    earlier = (iota((toks, toks), 0) < iota((toks, toks), 1)).astype(F32).astype(BF16)
    named16 = named.astype(BF16)
    rank16 = dot(named16, earlier).astype(BF16)
    score_high = score.astype(BF16)
    rest = score - score_high.astype(F32)
    score_low = rest.astype(BF16)
    score_last = (rest - score_low.astype(F32)).astype(BF16)

    ones = jnp.ones((8, toks), BF16)
    load = dot_across(ones, named16)
    mass = dot_across(ones, score_high) + dot_across(ones, score_low) + dot_across(ones, score_last)
    row8 = iota((8, lanes), 0)
    stat_mine[0] = jnp.where(row8 == 0, load, jnp.where(row8 == 1, mass, 0.0))

    wide = 128
    slot_wide = (iota((toks, wide), 1) & 15).astype(F32)
    for z in range(ZH):
        pick = (iota((lanes, wide), 0) == expert_of(iota((lanes, wide), 1) >> 4, z)).astype(F32).astype(BF16)
        there = dot_down(rank16, pick) == slot_wide
        w_send[z, 0] = jnp.where(there, dot_down(score_high, pick), 0.0).astype(BF16)
        w_send[z, 1] = jnp.where(there, dot_down(score_low, pick), 0.0).astype(BF16)
        w_send[z, 2] = jnp.where(there, dot_down(named16, pick), 0.0).astype(BF16)

    starts(stat_a_copy, GROUPS)
    for k in range(1, ZH):
        w_copy(k).start()
    stat_a[dp] = stat_mine[0]
    w_recv[zh] = w_send[zh]

    ring_step(2)
    ring_step(3)
    relay(0)
    relay(1)
    for array in "gud":
        start_zx(array)

    ring_step(4)
    ring_step(5)

    all_of(w_recv.at[: ZH - 1], w_ssem.at[0], w_rsem.at[0]).wait_recv()
    from_slot, to_slot = iota((wide, slots), 0), iota((wide, slots), 1)
    for z in range(ZH):
        widen = (
            ((to_slot >> 6) == (from_slot >> 4))
            & (((to_slot >> 4) & 3) == z)
            & ((to_slot & 15) == (from_slot & 15))
        )
        widen = widen.astype(F32).astype(BF16)
        for kind in range(3):
            w_wide[pl.ds((kind * ZH + z) * toks, toks), :] = dot(w_recv[z, kind], widen).astype(BF16)

    rows_send(0)
    rows_send(1)
    ring_step(6)
    share(0)
    share(1)
    ring_step(7)
    ring_step(8)
    share(2)
    share(3)

    all_of(stat_a.at[: GROUPS - 1], sa_send.at[0], sa_recv.at[0]).wait_recv()
    stat_mine[1] = jnp.sum(stat_a[...], axis=0)
    starts(stat_b_copy, EXPERTS)
    stat_b[me] = stat_mine[1]

    for n in range(9, GATE_UP + 2):
        ring_step(n)

    rows_take(0)
    rows_take(1)
    for n in range(len(SHARED)):
        wait_share(n)
    for s in (RIGHT, LEFT):
        for n in range(GATE_UP):
            wait_ring(s, n)

    part_width = 256
    block = slots // 2
    def hidden_part(n, m):
        columns, at = slice(n * part_width, (n + 1) * part_width), slice(m * block, (m + 1) * block)
        gate = sum(
            dot(rows[k][at, :], gate_w[k * part : (k + 1) * part, columns]) for k in range(PARTS)
        )
        up = sum(dot(rows[k][at, :], up_w[k * part : (k + 1) * part, columns]) for k in range(PARTS))
        hidden[at, columns] = (gate / (1.0 + jnp.exp(-gate)) * up).astype(BF16)

    pieces = [(n, m) for n in range(hid // part_width) for m in range(slots // block)]
    for turn in range(2):
        for n, m in pieces[turn * len(pieces) // 2 : (turn + 1) * len(pieces) // 2]:
            hidden_part(n, m)
        ring_step(GATE_UP + 2 + turn)
        share_down(2 * turn)
        share_down(2 * turn + 1)

    def x_copy(n):
        def copy(k):
            to = (xc + k) % XC
            return remote(
                block_of(produced[n], to),
                block_of(x_in[n], xc),
                xp_send.at[n],
                xp_recv.at[n],
                dp,
                expert_index(to // C, zh, to % C),
            )

        return copy

    def z_copy(n):
        def copy(k):
            to = (zh + k) % ZH
            return remote(
                partial[n].at[to],
                z_in[n].at[zh],
                zp_send.at[n],
                zp_recv.at[n],
                dp,
                expert_index(x, to, core),
            )

        return copy

    def wait_down(z, first, columns):
        needed = range(first // piece, -(-(first + columns) // piece))
        if z == 1 and 1 in needed:
            wait_zx("d")
        for away, part_of in SHARED_DOWN:
            if z == 1 and (away + 1) % Y in needed:
                wait_share_down(away, part_of)
        for s in (RIGHT, LEFT):
            for m in range(GATE_UP, MESSAGES):
                if order[s][m][1] == z and (1 - s * (order[s][m][2] + 1)) % Y in needed:
                    wait_ring(s, m)

    def produce(n):
        z, first, columns = CHUNKS[n]
        wait_down(z, first, columns)
        produced[n][...] = dot_across(
            hidden[...], down_w[pl.ds(z * Y * piece + first, columns), :]
        ).astype(BF16)
        starts(x_copy(n), XC)
        at = pl.ds(pl.multiple_of(xc * ZH * CAP, ZH * CAP), ZH * CAP)
        x_in[n][at, :] = produced[n][at, :]

    def combine(n):
        all_of(x_in[n].at[: (XC - 1) * ZH * CAP], xp_send.at[n], xp_recv.at[n]).wait_recv()
        both = dot(w_wide[: 2 * ZH * toks, :], x_in[n][...])
        summed = (both[: ZH * toks] + both[ZH * toks :]).astype(BF16)
        for z in range(ZH):
            partial[n][z] = summed[z * toks : (z + 1) * toks]
        starts(z_copy(n), ZH)
        z_in[n][zh] = partial[n][zh]

    def finish(n):
        all_of(z_in[n].at[: ZH - 1], zp_send.at[n], zp_recv.at[n]).wait_recv()
        result = z_in[n][0].astype(F32)
        for z in range(1, ZH):
            result = result + z_in[n][z].astype(F32)
        z, first, columns = CHUNKS[n]
        relative[z, :, first : first + columns] = result

    def place_columns(z):
        there = pl.multiple_of((zl if z == 0 else 1 - zl) * Y * piece, Y * piece)
        turned = pltpu.roll(relative[z], ((y + Y - 1) % Y) * piece, 1)
        out[:, pl.ds(there, Y * piece)] = turned.astype(BF16)

    produce(0)
    produce(1)
    ring_step(GATE_UP + 4)
    combine(0)
    ring_step(GATE_UP + 5)
    produce(2)
    ring_step(GATE_UP + 6)
    combine(1)
    ring_step(GATE_UP + 7)
    ring_step(GATE_UP + 8)
    produce(4)
    produce(3)
    combine(2)
    produce(5)
    ring_step(GATE_UP + 9)
    combine(4)
    ring_step(GATE_UP + 10)
    combine(3)
    produce(6)
    ring_step(GATE_UP + 11)
    finish(0)
    finish(1)
    combine(5)
    produce(7)
    finish(2)
    combine(6)
    produce(8)
    produce(9)
    all_of(stat_b.at[: EXPERTS - 1], sb_send.at[0], sb_recv.at[0]).wait_recv()
    totals = jnp.sum(stat_b[...], axis=0)
    count, masses = totals[0:1, :], totals[1:2, :]
    total = toks * GROUPS * EXPERTS
    loss = jnp.sum(
        (EXPERTS * count / (topk * total)) * (masses / total), axis=1, keepdims=True
    )
    my_load = jnp.sum(jnp.where(iota((1, lanes), 1) == me, count, 0.0), axis=1, keepdims=True)
    load_out[...] = my_load.astype(I32)
    loss_out[...] = loss

    combine(7)
    combine(8)
    combine(9)
    finish(3)
    finish(4)
    finish(5)
    place_columns(0)
    for n in range(6, len(CHUNKS)):
        finish(n)
    place_columns(1)

    for s in (0, 1):
        all_of(gate_w.at[: GATE_UP * piece], ring_send.at[s, 0], ring_recv.at[s, 0]).wait_send()
        all_of(
            down_w.at[: (MESSAGES - GATE_UP) * half], ring_send.at[s, 1], ring_recv.at[s, 0]
        ).wait_send()
    all_of(gate_w.at[: 3 * piece], zx_send.at[0], zx_recv.at[0]).wait_send()
    all_of(gate_w.at[: len(SHARED) * piece], share_send.at[0], share_recv.at[0]).wait_send()
    all_of(down_w.at[: len(SHARED_DOWN) * half], share_send.at[1], share_recv.at[0]).wait_send()
    all_of(w_recv.at[: ZH - 1], w_ssem.at[0], w_rsem.at[0]).wait_send()
    all_of(stat_a.at[: GROUPS - 1], sa_send.at[0], sa_recv.at[0]).wait_send()
    all_of(stat_b.at[: EXPERTS - 1], sb_send.at[0], sb_recv.at[0]).wait_send()
    for n in range(PARTS):
        all_of(token_all[n].at[: (ZH - 1) * toks], token_send.at[n], token_recv.at[n, 0]).wait_send()
        all_of(rows[n].at[: (XC - 1) * ZH * CAP], row_send.at[n], row_recv.at[n]).wait_send()
    for n in range(len(CHUNKS)):
        all_of(x_in[n].at[: (XC - 1) * ZH * CAP], xp_send.at[n], xp_recv.at[n]).wait_send()
        all_of(z_in[n].at[: ZH - 1], zp_send.at[n], zp_recv.at[n]).wait_send()


def on_device(tokens, expert_ids, gate_scores, w_gate, w_up, w_down):
    toks, width = tokens.shape
    hid = w_gate.shape[2]
    slots = EXPERTS * CAP
    dma = pltpu.SemaphoreType.DMA
    vmem = pl.BlockSpec(memory_space=pltpu.VMEM)
    mixed, load, loss = pl.pallas_call(
        kernel,
        out_shape=(
            jax.ShapeDtypeStruct((toks, width), BF16),
            jax.ShapeDtypeStruct((1, 1), I32),
            jax.ShapeDtypeStruct((1, 1), F32),
        ),
        in_specs=[pl.BlockSpec(memory_space=pl.ANY)] * 6,
        out_specs=(vmem, vmem, vmem),
        scratch_shapes=[
            pltpu.VMEM(expert_ids.shape[::-1], I32),
            pltpu.VMEM(expert_ids.shape[::-1], F32),
            pltpu.VMEM((width, hid), BF16),
            pltpu.VMEM((width, hid), BF16),
            pltpu.VMEM((width, hid), BF16),
            pltpu.VMEM((slots, hid), BF16),
            pltpu.VMEM((ZL, toks, width // ZL), F32),
            pltpu.VMEM((ZH, 3, toks, 128), BF16),
            pltpu.VMEM((ZH, 3, toks, 128), BF16),
            pltpu.VMEM((3 * ZH * toks, slots), BF16),
            pltpu.VMEM((GROUPS, 8, 128), F32),
            pltpu.VMEM((EXPERTS, 8, 128), F32),
            pltpu.VMEM((2, 8, 128), F32),
            dma((7,)),
            dma((2, 2)),
            dma((2, MESSAGES)),
            dma((1,)),
            dma((3,)),
            dma((2,)),
            dma((len(SHARED) + len(SHARED_DOWN),)),
            dma((PARTS,)),
            dma((PARTS, ZH)),
            dma((PARTS,)),
            dma((PARTS,)),
            dma((1,)),
            dma((1,)),
            dma((1,)),
            dma((1,)),
            dma((1,)),
            dma((1,)),
            dma((len(CHUNKS),)),
            dma((len(CHUNKS),)),
            dma((len(CHUNKS),)),
            dma((len(CHUNKS),)),
        ]
        + [pltpu.VMEM((toks, width // PARTS), BF16)] * PARTS
        + [pltpu.VMEM((ZH * toks, width // PARTS), BF16)] * PARTS
        + [pltpu.VMEM((slots, width // PARTS), BF16)] * (2 * PARTS)
        + [pltpu.VMEM((slots, w), BF16) for _, _, w in CHUNKS] * 2
        + [pltpu.VMEM((ZH, toks, w), BF16) for _, _, w in CHUNKS] * 2,
        compiler_params=pltpu.CompilerParams(
            collective_id=0, has_side_effects=True, vmem_limit_bytes=60 * 1024 * 1024
        ),
        name="routed_layer",
    )(tokens, expert_ids.T, gate_scores.T, w_gate[0], w_up[0], w_down[0].T)
    return mixed, load[0], loss[0, 0]


def solution(mesh):
    both = ("dp", "expert")
    return jax.shard_map(
        on_device,
        mesh=mesh,
        in_specs=(
            P(both, None),
            P(both, None),
            P(both, None),
            P("expert", "dp", None),
            P("expert", "dp", None),
            P("expert", None, "dp"),
        ),
        out_specs=(P(both, None), P("expert"), P()),
        check_vma=False,
    )
```
